256 devices in a mesh: occ: 16 (over z_lo, x), vir: 16 (over z_hi, y, core).
Axes of the slice: x: 4, y: 4, z: 8 (z_hi: 2, z_lo: 4; z = z_hi * 4 + z_lo), core: 2. Of those that a mesh axis runs over, the one named last changes fastest.
Arguments:
- b_occ: bfloat16 [64, 768, 2304], P('occ', 'vir'), may hold values from -0.86328125 to 0.86328125
- b_outer: bfloat16 [2, 768, 2304], P(None, 'vir', 'occ'), may hold values from -0.86328125 to 0.86328125
- eps_occ: float32 [64], P('occ'), may hold values from -1.5 to -0.3
- eps_outer: float32 [2], replicated, may hold values from -1.5 to -0.3
- eps_vir: float32 [768], P('vir'), may hold values from 0.2 to 3
Outputs:
- gamma_occ: float32 [64, 768, 2304], P('occ', 'vir')
- gamma_outer: float32 [2, 768, 2304], P(None, 'vir', 'occ')
The draws below stay inside these ranges and needn't reach their ends.
All inputs are finite; a program needn't handle non-finite values.
Results may differ from the reference program's by a relative error of at most 0.0018.
Values may be sent and summed in bfloat16 or wider, within the bound.
No kernel may reach another device: no remote copies, remote signals or barrier semaphores. Data moves between devices by JAX's collectives and lax.ppermute only.
A program may use at most 128 MiB of HBM per device.

```python
import jax
import jax.numpy as jnp
from jax import lax

V = 768
P_SIZE = 2304
NJ = 2
NI = 64


def spiked(array, own_key, source, target, parts, factor):
    def block_of(position):
        return (jnp.arange(array.shape[position]) // (array.shape[position] // parts)).reshape((-1,) + (1,) * (array.ndim - 1 - position))

    one_side = jax.random.permutation(own_key, parts)[block_of(target)]
    other_side = (block_of(target) + parts // 2) % parts
    return jnp.where((block_of(source) == one_side) | (block_of(source) == other_side), factor * array, array)


def level_of(stream_key, shape, cuts, smallest, top_value):
    gain, own = 1.0, jax.random.fold_in(stream_key, 6)
    for position, blocks in cuts:
        steps = jnp.exp(jax.random.uniform(jax.random.fold_in(own, position), (blocks,), jnp.float32, smallest / len(cuts), top_value / len(cuts)))
        gain = gain * jnp.repeat(steps, shape[position] // blocks).reshape([-1 if axis == position else 1 for axis in range(len(shape))])
    return gain


def gaussian(key, extent, scale, bound, cuts=(), held_as=jnp.bfloat16):
    level = level_of(key, extent, cuts, -0.22, 0.18) if cuts else 1.0
    entries = jax.random.normal(key, extent, jnp.float32) * scale * level
    return jnp.minimum(jnp.maximum(entries, -bound), bound).astype(held_as)


def bell_draw_with(rng, shape, scale, reach, split, heavy, held_as=jnp.bfloat16):
    array = scale * jax.random.normal(rng, shape, jnp.float32)
    if split:
        array = array * level_of(rng, shape, split, -0.22, 0.18)
    return jnp.clip(spiked(array, jax.random.fold_in(rng, 3), *heavy), -reach, reach).astype(held_as)


def setup_inputs(seed: int = 0) -> dict:
    seeds = jax.random.split(jax.random.key(seed), 6)
    b_occ = bell_draw_with(seeds[0], (NI, V, P_SIZE), (P_SIZE ** -0.25), 0.86328125, ((0, 16), (1, 16)), (0, 2, 16, 2.0))
    b_outer = gaussian(seeds[1], (NJ, V, P_SIZE), (P_SIZE ** -0.25), 0.86328125, ((1, 16), (2, 16)))
    eps_occ = jnp.clip(-1.5 + 1.2 * jax.random.uniform(seeds[2], (NI,), jnp.float32) ** level_of(seeds[2], (NI,), ((0, 16),), -0.2, 0.2), -1.5, -0.3)
    eps_outer = jnp.clip(jax.random.uniform(seeds[3], (NJ,), jnp.float32, -1.5, -0.3), -1.5, -0.3)
    eps_vir = jnp.clip(0.2 + 2.8 * jax.random.uniform(seeds[4], (V,), jnp.float32) ** level_of(seeds[4], (V,), ((0, 16),), -0.2, 0.2), 0.2, 3.0)
    return dict(b_occ=b_occ, b_outer=b_outer, eps_occ=eps_occ, eps_outer=eps_outer, eps_vir=eps_vir)


def reference(b_occ, b_outer, eps_occ, eps_outer, eps_vir):
    flat = b_occ.reshape(NI * V, P_SIZE)
    flat_wide = flat.astype(jnp.float32)
    gamma_occ = jnp.zeros((NI * V, P_SIZE), jnp.float32)
    results = []
    for jpos in range(NJ):
        integral = jnp.dot(flat, b_outer[jpos].T, preferred_element_type=jnp.float32).reshape(NI, V, V)
        denom = eps_occ[:, None, None] + eps_outer[jpos] - eps_vir[None, :, None] - eps_vir[None, None, :]
        amps = integral / denom
        tilde = (2.0 * amps - jnp.swapaxes(amps, 1, 2)).reshape(NI * V, V)
        outer_wide = b_outer[jpos].astype(jnp.float32)
        gamma_occ = gamma_occ + jnp.dot(tilde, outer_wide, precision=lax.Precision.HIGHEST)
        results.append(jnp.dot(tilde.T, flat_wide, precision=lax.Precision.HIGHEST))
    return gamma_occ.reshape(NI, V, P_SIZE), jnp.stack(results)
```

```python
import jax
import jax.numpy as jnp
from jax import lax
from jax.sharding import Mesh
from jax.sharding import PartitionSpec as P

AXES = ("zl", "x", "zh", "y", "core")
SIZES = (4, 4, 2, 4, 2)
NX, NY, NZL, NZH = 4, 4, 4, 2
BF, F16, F32 = jnp.bfloat16, jnp.float16, jnp.float32
EXTRA = 16


def rounded(x):
    return lax.reduce_precision(x, 8, 7)


def shift(array, axis, k, size):
    return lax.ppermute(array, axis, [(p, (p + k) % size) for p in range(size)])


def pieces3(x):
    hi = rounded(x)
    mid = rounded(x - hi)
    return hi, mid, x - hi - mid


def ring_blocks(array, axis, size):
    return [array] + [shift(array, axis, k, size) for k in range(1, size)]


def ring_sum(blocks, axis, size, scale):
    total = blocks[0].astype(F32)
    for k in range(1, size):
        total = total + shift(blocks[k], axis, size - k, size).astype(F32)
    return total * scale


def blocks_behind(array, dim, here, size):
    return [lax.dynamic_index_in_dim(array, (here - k) % size, dim, keepdims=False) for k in range(size)]


def on_device(b_occ, b_outer, eps_occ, eps_outer, eps_vir):
    ni, na, nq = b_occ.shape
    nqo = b_outer.shape[2]
    core, xi, zh = lax.axis_index("core"), lax.axis_index("x"), lax.axis_index("zh")
    wide = 128 * -(-(NZL * nqo + 3 * 16) // 128)
    chip = 2 * na

    other_rows = lax.ppermute(b_occ, "core", [(0, 1), (1, 0)])

    occ_top = jnp.max(jnp.abs(b_occ)).astype(BF)
    row_top = jnp.max(jnp.abs(b_outer), axis=2)
    e0, e1, e2 = (p.astype(BF) for p in pieces3(eps_vir))
    side = jnp.stack([jnp.broadcast_to(e, (2, na)) for e in (e0, e1, e2)] + [jnp.full((2, na), occ_top), row_top], axis=2)
    message = jnp.concatenate([b_outer, side, jnp.zeros((2, na, EXTRA - 5), BF)], axis=2)
    mine = lax.all_to_all(message, "core", 0, 0, tiled=True).reshape(chip, nqo + EXTRA)

    along_z = lax.all_to_all(
        jnp.broadcast_to(mine[None], (NZH * NZL, *mine.shape)), ("zh", "zl"), 0, 0, tiled=True
    ).reshape(NZH, NZL, chip, nqo + EXTRA)
    data = jnp.moveaxis(along_z[..., :nqo], 1, 2).reshape(NZH, chip, NZL * nqo)
    extras = jnp.concatenate([along_z[:, 0, :, nqo:], jnp.max(along_z[..., nqo:], axis=1)], axis=-1)
    pad = wide - NZL * nqo - 2 * EXTRA
    both = jnp.concatenate([data, extras, jnp.zeros((NZH, chip, pad), BF)], axis=2)
    near = jnp.where(zh == 0, both[0], both[1])
    far = jnp.where(zh == 0, both[1], both[0])

    near_x = jnp.concatenate(ring_blocks(near, "x", NX), axis=1)
    far_y = jnp.concatenate(ring_blocks(far, "y", NY), axis=0)
    near_all = jnp.concatenate(ring_blocks(near_x, "y", NY), axis=0)
    far_all = jnp.concatenate(ring_blocks(far_y, "x", NX), axis=1)
    b_all = jnp.concatenate([near_all, far_all], axis=0)
    nv = b_all.shape[0]

    pair = jnp.where(core == 0, jnp.stack([b_occ, other_rows], 1), jnp.stack([other_rows, b_occ], 1))
    cols = pair.reshape(ni * chip, NZL, NX, nqo)
    cols = jnp.moveaxis(cols, 2, 1).reshape(ni * chip, NX, NZL * nqo)
    cols = jnp.pad(cols, ((0, 0), (0, 0), (0, wide - NZL * nqo)))
    occ_all = jnp.concatenate(blocks_behind(cols, 1, xi, NX), axis=1)

    tail = b_all.reshape(nv, NX, wide)[:, :, NZL * nqo : NZL * nqo + 2 * EXTRA].astype(F32)
    eps_all = tail[:, 0, 0] + tail[:, 0, 1] + tail[:, 0, 2]
    occ_max = jnp.max(tail[:, :, EXTRA + 3])
    outer_max = jnp.max(tail[:, :, EXTRA + 4])
    eps_here = lax.slice_in_dim(eps_all, 0, chip)
    eps_j = jnp.where(core == 0, eps_outer[0], eps_outer[1])
    eps_row = (eps_occ[:, None] + eps_j - eps_here[None, :]).reshape(ni * chip)

    amp_top = jnp.maximum(nq * occ_max * outer_max, 1e-30)
    amp_scale = 60000.0 / amp_top
    sum_top = jnp.maximum(3.0 * ni * chip * amp_top * occ_max, 1e-30)
    sum_scale = 60000.0 / sum_top

    integral = jnp.einsum("rq,bq->rb", occ_all, b_all, preferred_element_type=F32)
    amps = integral / (eps_row[:, None] - eps_all[None, :])
    integral_t = jnp.einsum("bq,rq->br", b_all, occ_all, preferred_element_type=F32)
    amps_t = integral_t / (eps_row[None, :] - eps_all[:, None])

    sent = (amps * amp_scale).astype(F16).reshape(ni, chip, NZH, NY, chip)
    got = []
    for s in range(NZH):
        for k in range(NY):
            block = sent[:, :, s, (-k) % NY]
            if s or k:
                pairs = [
                    (h * NY + y, (h ^ s) * NY + (y + k) % NY) for h in range(NZH) for y in range(NY)
                ]
                block = lax.ppermute(block, ("zh", "y"), pairs)
            got.append(block)
    got = jnp.stack(got, 0)
    swapped_t = jnp.moveaxis(got, 1, 2).reshape(nv, ni * chip).astype(F32) * (1.0 / amp_scale)
    tilde_t = 2.0 * amps_t - swapped_t
    hi32 = rounded(tilde_t)
    hi, lo = hi32.astype(BF), (tilde_t - hi32).astype(BF)

    partial = (
        jnp.einsum("br,rq->bq", hi, occ_all, preferred_element_type=F32)
        + jnp.einsum("br,rq->bq", lo, occ_all, preferred_element_type=F32)
    )
    half = nv // NZH
    packed = (partial * sum_scale).astype(F16)
    near_rows = [packed[k * chip : (k + 1) * chip] for k in range(NY)]
    far_cols = [packed[half:, k * wide : (k + 1) * wide] for k in range(NX)]
    near_s = ring_sum(near_rows, "y", NY, 0.25).astype(F16)
    far_s = ring_sum(far_cols, "x", NX, 0.25).astype(F16)
    near_t = ring_sum([near_s[:, k * wide : (k + 1) * wide] for k in range(NX)], "x", NX, 0.25).astype(F16)
    far_t = ring_sum([far_s[k * chip : (k + 1) * chip] for k in range(NY)], "y", NY, 0.25).astype(F16)
    halves = jnp.where(zh == 0, jnp.stack([near_t, far_t]), jnp.stack([far_t, near_t]))
    tiles = halves[:, :, : NZL * nqo].reshape(NZH, chip, NZL, nqo)
    tiles = jnp.moveaxis(tiles, 2, 1).reshape(NZH * NZL, chip, nqo)
    arrived = lax.all_to_all(tiles, ("zh", "zl"), 0, 0, tiled=True)
    section = arrived.astype(F32).sum(0) * (16.0 / sum_scale)
    gamma_outer = lax.all_to_all(section.reshape(2, na, nqo), "core", 0, 0, tiled=True)

    rows = (
        jnp.einsum("br,bq->rq", hi, b_all, preferred_element_type=F32)
        + jnp.einsum("br,bq->rq", lo, b_all, preferred_element_type=F32)
    ).reshape(ni, 2, na, NX * wide)
    keep = jnp.where(core == 0, rows[:, 0], rows[:, 1])
    give = jnp.where(core == 0, rows[:, 1], rows[:, 0])
    total = keep + lax.ppermute(give, "core", [(0, 1), (1, 0)])
    total = total.reshape(ni, na, NX, wide)[..., : NZL * nqo].reshape(ni, na, NX, NZL, nqo)
    ordered = jnp.stack(blocks_behind(total, 2, xi, NX), axis=3)
    gamma_occ = ordered.reshape(ni, na, nq)
    return (gamma_occ, gamma_outer)


def solution(mesh):
    fine = Mesh(mesh.devices.reshape(SIZES), AXES)
    occ, vir = ("zl", "x"), ("zh", "y", "core")
    return jax.shard_map(
        on_device,
        mesh=fine,
        in_specs=(P(occ, vir, None), P(None, vir, occ), P(occ), P(), P(vir)),
        out_specs=(P(occ, vir, None), P(None, vir, occ)),
        check_vma=False,
    )
```

```python
import jax
import jax.numpy as jnp
from jax import lax
from jax.experimental import pallas as pl
from jax.experimental.pallas import tpu as pltpu
from jax.sharding import Mesh
from jax.sharding import PartitionSpec as P

AXES = ("zl", "x", "zh", "y", "core")
SIZES = (4, 4, 2, 4, 2)
NX, NY, NZL, NZH = 4, 4, 4, 2
NM = NZH * NY
BF, F16, F32 = jnp.bfloat16, jnp.float16, jnp.float32
EXTRA = 16
OCC_TOP, OUTER_TOP = 3, 4
LANES = 128
SMEM = pl.BlockSpec(memory_space=pltpu.SMEM)
VMEM = pl.BlockSpec(memory_space=pltpu.VMEM)
CORES = [(0, 1), (1, 0)]


def call(kernel, outs, scalars, *arrays):
    return pl.pallas_call(
        kernel,
        out_shape=[jax.ShapeDtypeStruct(s, d) for s, d in outs],
        in_specs=[SMEM] + [VMEM] * len(arrays),
        out_specs=[VMEM] * len(outs),
        compiler_params=pltpu.CompilerParams(vmem_limit_bytes=48 * 2**20),
    )(jnp.stack(scalars).astype(jnp.int32), *arrays)


def shift(array, axis, k, size):
    return lax.ppermute(array, axis, [(p, (p + k) % size) for p in range(size)])


def nt(a, b):
    return lax.dot_general(a, b, (((1,), (1,)), ((), ())), preferred_element_type=F32)


def message_kernel(s, occ, outer, eps, keep, give):
    core = s[0]
    occ_top = jnp.max(jnp.abs(occ[...].astype(F32)))
    e = eps[...]
    parts = []
    for _ in range(3):
        part = e.astype(BF).astype(F32)
        parts.append(part)
        e = e - part
    na, nqo = outer.shape[1:]
    lane = lax.broadcasted_iota(jnp.int32, (na, EXTRA), 1)
    for out, j in ((keep, core), (give, 1 - core)):
        rows = outer[j]
        row_top = jnp.max(jnp.abs(rows.astype(F32)), axis=1, keepdims=True)
        side = jnp.where(lane == OCC_TOP, occ_top, 0.0)
        for n, part in enumerate(parts):
            side = jnp.where(lane == n, part, side)
        side = jnp.where(lane == OUTER_TOP, row_top, side)
        out[:, :nqo] = rows
        out[:, nqo:] = side.astype(BF)


def lay_out_kernel(s, z, near, far):
    zh = s[0]
    nqo = z.shape[2] - EXTRA
    rows, wide = near.shape
    for out, half in ((near, zh), (far, 1 - zh)):
        blocks = [z[half * NZL + k] for k in range(NZL)]
        most = blocks[0][:, nqo:]
        for b in blocks[1:]:
            most = jnp.maximum(most, b[:, nqo:])
        used = NZL * nqo + 2 * EXTRA
        out[...] = jnp.concatenate(
            [b[:, :nqo] for b in blocks] + [blocks[0][:, nqo:], most, jnp.zeros((rows, wide - used), BF)], axis=1
        )


def occ_kernel(s, own, other, out):
    xi = s[0]
    ni, na, nq = own.shape
    nqo, wide = nq // (NX * NZL), out.shape[2]
    for xa in range(NX):
        kx = (xi - xa) & (NX - 1)
        for i in range(ni):
            for c, src in enumerate((own, other)):
                cols = [src[i, :, (zl * NX + xa) * nqo : (zl * NX + xa + 1) * nqo] for zl in range(NZL)]
                cols.append(jnp.zeros((na, wide - NZL * nqo), BF))
                at = (2 * i + c) * na
                out[kx, at : at + na, :] = jnp.concatenate(cols, axis=1)


def amps_kernel(ni, nqo, s, n0, n1, n3, n2a, n2b, f0, f1, f3, f2a, f2b, occ, eps_lane, eps_sub, b_all, at, send, scales):
    zh, y = s[0], s[1]
    chip = n0.shape[1]
    half = NY * chip
    for kx in range(NX):
        two = (n2a, n2b)[kx // 2]
        for ky, piece in enumerate((n0[kx], n1[kx], two[kx % 2], n3[kx])):
            b_all[kx, ky * chip : (ky + 1) * chip, :] = piece
    for ky in range(NY):
        two = (f2a, f2b)[ky // 2]
        for kx, piece in enumerate((f0[ky], f1[ky], two[ky % 2], f3[ky])):
            b_all[kx, half + ky * chip : half + (ky + 1) * chip, :] = piece
    tile = NZL * nqo // LANES * LANES
    off = NZL * nqo - tile
    tail = b_all[0, :, tile : tile + LANES].astype(F32)
    eps_b_sub = tail[:, off : off + 1] + tail[:, off + 1 : off + 2] + tail[:, off + 2 : off + 3]
    lane8 = lax.broadcasted_iota(jnp.int32, (8, LANES), 1)
    pick = jnp.where((lane8 >= off) & (lane8 < off + 3), 1.0, 0.0).astype(BF)
    eps_b_lane = nt(pick, b_all[0, :, tile : tile + LANES])[0:1]
    most = jnp.max(tail, axis=0, keepdims=True)
    for kx in range(1, NX):
        most = jnp.maximum(most, jnp.max(b_all[kx, :, tile : tile + LANES].astype(F32), axis=0, keepdims=True))
    lane1 = lax.broadcasted_iota(jnp.int32, (1, LANES), 1)

    def extra(n):
        return jnp.sum(jnp.where(lane1 == off + EXTRA + n, most, 0.0), axis=1, keepdims=True)

    nq = NX * NZL * nqo
    amp_top = jnp.maximum(nq * extra(OCC_TOP) * extra(OUTER_TOP), 1e-30)
    sum_top = jnp.maximum(3.0 * ni * chip * amp_top * extra(OCC_TOP), 1e-30)
    amp_scale, sum_scale = 60000.0 / amp_top, 15000.0 / sum_top
    for n, value in enumerate((amp_scale, amp_top / 60000.0, sum_scale, sum_top / 15000.0)):
        scales[n : n + 1, :] = jnp.broadcast_to(value, (1, LANES))

    total = nt(occ[0], b_all[0])
    total_t = nt(b_all[0], occ[0])
    for kx in range(1, NX):
        total = total + nt(occ[kx], b_all[kx])
        total_t = total_t + nt(b_all[kx], occ[kx])
    at[...] = total_t / (eps_lane[...] - eps_b_sub)
    scaled = total / (eps_sub[...] - eps_b_lane) * amp_scale
    for h in range(NZH):
        for k in range(NY):
            m, to = h * NY + k, (zh ^ h) * NY + ((y - k) & (NY - 1))
            send[to] = jnp.concatenate(
                [scaled[i * chip : (i + 1) * chip, m * chip : (m + 1) * chip] for i in range(ni)], axis=1
            )


def tilde_kernel(s, at, st, occ, scales, hi, lo, near, far):
    zh, y = s[0], s[1]
    chip = st.shape[1]
    back, scale = scales[1:2, 0:1], scales[2:3, 0:1]
    for h in range(NZH):
        for k in range(NY):
            m, to = h * NY + k, (zh ^ h) * NY + ((y - k) & (NY - 1))
            t = 2.0 * at[m * chip : (m + 1) * chip, :] - st[to] * back
            top = t.astype(BF)
            hi[m * chip : (m + 1) * chip, :] = top
            lo[m * chip : (m + 1) * chip, :] = (t - top.astype(F32)).astype(BF)
    for kx in range(NX):
        part = jnp.dot(hi[...], occ[kx], preferred_element_type=F32)
        part = (part + jnp.dot(lo[...], occ[kx], preferred_element_type=F32)) * scale
        for ky in range(NY):
            near[ky, kx] = part[ky * chip : (ky + 1) * chip]
            far[kx, ky] = part[(NY + ky) * chip : (NY + ky + 1) * chip]


def gamma_occ_kernel(s, hi, lo, b_all, keep, give):
    xi = s[0]
    ni, na, nq = keep.shape
    nqo = nq // (NX * NZL)
    hi_t, lo_t = hi[...].T, lo[...].T
    for xa in range(NX):
        b = b_all[(xi - xa) & (NX - 1)]
        rows = jnp.dot(hi_t, b, preferred_element_type=F32) + jnp.dot(lo_t, b, preferred_element_type=F32)
        for i in range(ni):
            for c, out in enumerate((keep, give)):
                block = rows[(2 * i + c) * na : (2 * i + c + 1) * na]
                for zl in range(NZL):
                    q = (zl * NX + xa) * nqo
                    out[i, :, q : q + nqo] = block[:, zl * nqo : (zl + 1) * nqo]


def ring_gather(array, axis):
    b1, b3 = shift(array, axis, 1, 4), shift(array, axis, 3, 4)
    return b1, b3, shift(b1[:2], axis, 1, 4), shift(b3[2:], axis, 3, 4)


def ring_sum_first(blocks, axis):
    c1, c2, c3 = blocks[1], blocks[2].astype(F16), blocks[3]
    r1, r3 = shift(c2[:2], axis, 3, 4), shift(c2[2:], axis, 1, 4)
    c1 = jnp.concatenate([c1[:2] + r1.astype(F32), c1[2:]]).astype(F16)
    c3 = jnp.concatenate([c3[:2], c3[2:] + r3.astype(F32)]).astype(F16)
    return c1, c3


def ring_sum_second(c0, c1, c3, axis):
    return c0 + shift(c1, axis, 3, 4).astype(F32) + shift(c3, axis, 1, 4).astype(F32)


def sum_direct(blocks, axis):
    total = blocks[0].astype(F32)
    for k in range(1, 4):
        total = total + shift(blocks[k], axis, 4 - k, 4).astype(F32)
    return total


def on_device(b_occ, b_outer, eps_occ, eps_outer, eps_vir):
    ni, na, nq = b_occ.shape
    nqo = b_outer.shape[2]
    core, xi, zh, y = (lax.axis_index(n) for n in ("core", "x", "zh", "y"))
    wide = LANES * -(-(NZL * nqo + 2 * EXTRA) // LANES)
    chip = 2 * na
    rows, nv = ni * chip, NM * chip

    keep, give = call(
        message_kernel, [((na, nqo + EXTRA), BF)] * 2, [core], b_occ, b_outer, eps_vir.reshape(na, 1)
    )
    mine = jnp.concatenate([keep, lax.ppermute(give, "core", CORES)], axis=0)

    along_z = lax.all_to_all(jnp.broadcast_to(mine[None], (NZH * NZL, *mine.shape)), ("zh", "zl"), 0, 0, tiled=True)
    near, far = call(lay_out_kernel, [((chip, wide), BF)] * 2, [zh], along_z)

    near_x = jnp.stack([near] + [shift(near, "x", k, NX) for k in range(1, NX)])
    far_y = jnp.stack([far] + [shift(far, "y", k, NY) for k in range(1, NY)])
    near_all = ring_gather(near_x, "y")
    far_all = ring_gather(far_y, "x")

    other_rows = lax.ppermute(b_occ, "core", CORES)
    (occ_all,) = call(occ_kernel, [((NX, rows, wide), BF)], [xi], b_occ, other_rows)

    eps_here = jnp.sum(mine[:, nqo : nqo + 3].astype(F32), axis=1)
    eps_j = jnp.where(core == 0, eps_outer[0], eps_outer[1])
    eps_row = (eps_occ[:, None] + eps_j - eps_here[None, :]).reshape(rows)

    b_all, amps_t, scaled, scales = call(
        lambda *refs: amps_kernel(ni, nqo, *refs),
        [((NX, nv, wide), BF), ((nv, rows), F32), ((NM, chip, rows), F32), ((8, LANES), F32)],
        [zh, y], near_x, *near_all, far_y, *far_all, occ_all, eps_row[None, :], eps_row[:, None],
    )
    swapped_t = lax.all_to_all(scaled.astype(F16), ("zh", "y"), 0, 0, tiled=True).astype(F32)
    hi, lo, near_p, far_p = call(
        tilde_kernel,
        [((nv, rows), BF)] * 2 + [((NY, NX, chip, wide), F32), ((NX, NY, chip, wide), F32)],
        [zh, y], amps_t, swapped_t, occ_all, scales,
    )

    n1, n3 = ring_sum_first(near_p, "y")
    f1, f3 = ring_sum_first(far_p, "x")
    n1, n3, f1, f3, hi, lo = lax.optimization_barrier((n1, n3, f1, f3, hi, lo))
    near_s = (ring_sum_second(near_p[0], n1, n3, "y") * 0.25).astype(F16)
    far_s = (ring_sum_second(far_p[0], f1, f3, "x") * 0.25).astype(F16)

    kept, given = call(gamma_occ_kernel, [((ni, na, nq), F32)] * 2, [xi], hi, lo, b_all)
    gamma_occ = kept + lax.ppermute(given, "core", CORES)
    near_s, far_s, gamma_occ = lax.optimization_barrier((near_s, far_s, gamma_occ))

    near_t = (sum_direct(near_s, "x") * 0.25).astype(F16)
    far_t = (sum_direct(far_s, "y") * 0.25).astype(F16)
    halves = jnp.where(zh == 0, jnp.stack([near_t, far_t]), jnp.stack([far_t, near_t]))
    tiles = halves[:, :, : NZL * nqo].reshape(NZH, chip, NZL, nqo)
    tiles = jnp.moveaxis(tiles, 2, 1).reshape(NZH * NZL, chip, nqo)
    arrived = lax.all_to_all(tiles, ("zh", "zl"), 0, 0, tiled=True)
    section = arrived.astype(F32).sum(0) * (16.0 * scales[3, 0])
    mine_j, other_j = section[:na], lax.ppermute(section[na:], "core", CORES)
    gamma_outer = jnp.where(core == 0, jnp.stack([mine_j, other_j]), jnp.stack([other_j, mine_j]))
    return (gamma_occ, gamma_outer)


def solution(mesh):
    fine = Mesh(mesh.devices.reshape(SIZES), AXES)
    occ, vir = ("zl", "x"), ("zh", "y", "core")
    return jax.shard_map(
        on_device,
        mesh=fine,
        in_specs=(P(occ, vir, None), P(None, vir, occ), P(occ), P(), P(vir)),
        out_specs=(P(occ, vir, None), P(None, vir, occ)),
        check_vma=False,
    )
```

```python
import functools
import math

import jax
import jax.numpy as jnp
from jax import lax
from jax.experimental import pallas as pl
from jax.experimental.pallas import tpu as pltpu
from jax.sharding import Mesh
from jax.sharding import PartitionSpec as P

AXES = ("zl", "x", "zh", "y", "core")
SIZES = (4, 4, 2, 4, 2)
NX, NY, NZL, NZH = 4, 4, 4, 2
NM = NZH * NY
BF, F16, F32 = jnp.bfloat16, jnp.float16, jnp.float32
EXTRA = 16
OCC_TOP, OUTER_TOP = 3, 4
LANES = 128
SMEM = pl.BlockSpec(memory_space=pltpu.SMEM)
VMEM = pl.BlockSpec(memory_space=pltpu.VMEM)
CORES = [(0, 1), (1, 0)]


def call(kernel, outs, scalars, *arrays, flops=0, scratch=()):
    moved = sum(a.size * a.dtype.itemsize for a in arrays) + sum(4 * math.prod(s) for s, _ in outs)
    return pl.pallas_call(
        kernel,
        out_shape=[jax.ShapeDtypeStruct(s, d) for s, d in outs],
        in_specs=[SMEM] + [VMEM] * len(arrays),
        out_specs=[VMEM] * len(outs),
        scratch_shapes=list(scratch),
        cost_estimate=pl.CostEstimate(flops=flops, bytes_accessed=moved, transcendentals=0),
        compiler_params=pltpu.CompilerParams(vmem_limit_bytes=48 * 2**20),
    )(jnp.stack(scalars).astype(jnp.int32), *arrays)


def shift(array, axis, k, size):
    return lax.ppermute(array, axis, [(p, (p + k) % size) for p in range(size)])


def swap_z(array, t):
    flip = t % NZL * NZH + t // NZL
    return lax.ppermute(array, ("zl", "zh"), [(p, p ^ flip) for p in range(NZH * NZL)])


def nt(a, b):
    return lax.dot_general(a, b, (((1,), (1,)), ((), ())), preferred_element_type=F32)


def message_kernel(s, occ, outer, eps, keep, give):
    core = s[0]
    occ_top = jnp.max(jnp.abs(occ[...].astype(F32)))
    n = eps.shape[1]
    here = lax.broadcasted_iota(jnp.int32, (n, n), 0) == lax.broadcasted_iota(jnp.int32, (n, n), 1)
    e = jnp.sum(jnp.where(here, eps[...], 0.0), axis=1, keepdims=True)
    parts = []
    for _ in range(3):
        part = e.astype(BF).astype(F32)
        parts.append(part)
        e = e - part
    na, nqo = outer.shape[1:]
    lane = lax.broadcasted_iota(jnp.int32, (na, EXTRA), 1)
    for out, j in ((keep, core), (give, 1 - core)):
        rows = outer[j]
        row_top = jnp.max(jnp.abs(rows.astype(F32)), axis=1, keepdims=True)
        side = jnp.where(lane == OCC_TOP, occ_top, 0.0)
        for n, part in enumerate(parts):
            side = jnp.where(lane == n, part, side)
        side = jnp.where(lane == OUTER_TOP, row_top, side)
        out[:, :nqo] = rows
        out[:, nqo:] = side.astype(BF)


def lay_out_kernel(s, *refs):
    zl = s[0]
    pieces, (near, far, z) = refs[: NZH * NZL], refs[NZH * NZL :]
    for t, piece in enumerate(pieces):
        z[t // NZL * NZL + (zl ^ (t % NZL))] = piece[...]
    nqo = z.shape[2] - EXTRA
    rows, wide = near.shape
    for out, half in ((near, 0), (far, 1)):
        blocks = [z[half * NZL + k] for k in range(NZL)]
        most = blocks[0][:, nqo:]
        for b in blocks[1:]:
            most = jnp.maximum(most, b[:, nqo:])
        used = NZL * nqo + 2 * EXTRA
        out[...] = jnp.concatenate(
            [b[:, :nqo] for b in blocks] + [blocks[0][:, nqo:], most, jnp.zeros((rows, wide - used), BF)], axis=1
        )


def occ_kernel(s, own, other, out):
    xi = s[0]
    ni, na, nq = own.shape
    nqo, wide = nq // (NX * NZL), out.shape[2]
    for xa in range(NX):
        kx = (xi - xa) & (NX - 1)
        for i in range(ni):
            for c, src in enumerate((own, other)):
                cols = [src[i, :, (zl * NX + xa) * nqo : (zl * NX + xa + 1) * nqo] for zl in range(NZL)]
                cols.append(jnp.zeros((na, wide - NZL * nqo), BF))
                at = (2 * i + c) * na
                out[kx, at : at + na, :] = jnp.concatenate(cols, axis=1)


def amps_kernel(ni, nqo, s, *refs):
    zh, y = s[0], s[1]
    near, far, (occ, eps_lane, eps_sub, b_all, at, send, scales) = refs[:8], refs[8:16], refs[16:]
    chip = near[0].shape[1]
    half = NY * chip
    for k in range(4):
        for other in range(4):
            b_all[other, k * chip : (k + 1) * chip, :] = near[2 * k + other // 2][other % 2]
            at_row = half + other * chip
            b_all[k, at_row : at_row + chip, :] = far[2 * k + other // 2][other % 2]
    tile = NZL * nqo // LANES * LANES
    off = NZL * nqo - tile
    tail = b_all[0, :, tile : tile + LANES].astype(F32)
    eps_b_sub = tail[:, off : off + 1] + tail[:, off + 1 : off + 2] + tail[:, off + 2 : off + 3]
    lane8 = lax.broadcasted_iota(jnp.int32, (8, LANES), 1)
    pick = jnp.where((lane8 >= off) & (lane8 < off + 3), 1.0, 0.0).astype(BF)
    eps_b_lane = nt(pick, b_all[0, :, tile : tile + LANES])[0:1]
    most = jnp.max(tail, axis=0, keepdims=True)
    for kx in range(1, NX):
        most = jnp.maximum(most, jnp.max(b_all[kx, :, tile : tile + LANES].astype(F32), axis=0, keepdims=True))
    lane1 = lax.broadcasted_iota(jnp.int32, (1, LANES), 1)

    def extra(n):
        return jnp.sum(jnp.where(lane1 == off + EXTRA + n, most, 0.0), axis=1, keepdims=True)

    nq = NX * NZL * nqo
    amp_top = jnp.maximum(nq * extra(OCC_TOP) * extra(OUTER_TOP), 1e-30)
    sum_top = jnp.maximum(3.0 * ni * chip * amp_top * extra(OCC_TOP), 1e-30)
    amp_scale, sum_scale = 60000.0 / amp_top, 15000.0 / sum_top
    for n, value in enumerate((amp_scale, amp_top / 60000.0, sum_scale, sum_top / 15000.0)):
        scales[n : n + 1, :] = jnp.broadcast_to(value, (1, LANES))

    total = nt(occ[0], b_all[0])
    total_t = nt(b_all[0], occ[0])
    for kx in range(1, NX):
        total = total + nt(occ[kx], b_all[kx])
        total_t = total_t + nt(b_all[kx], occ[kx])
    at[...] = total_t / (eps_lane[...] - eps_b_sub)
    scaled = total / (eps_sub[...] - eps_b_lane) * amp_scale
    for h in range(NZH):
        for k in range(NY):
            m, to = h * NY + k, (zh ^ h) * NY + ((y - k) & (NY - 1))
            send[to] = jnp.concatenate(
                [scaled[i * chip : (i + 1) * chip, m * chip : (m + 1) * chip] for i in range(ni)], axis=1
            )


def tilde_kernel(s, at, st, occ, scales, hi, lo, near, far):
    zh, y = s[0], s[1]
    chip = st.shape[1]
    back, scale = scales[1:2, 0:1], scales[2:3, 0:1]
    for h in range(NZH):
        for k in range(NY):
            m, to = h * NY + k, (zh ^ h) * NY + ((y - k) & (NY - 1))
            t = 2.0 * at[m * chip : (m + 1) * chip, :] - st[to] * back
            top = t.astype(BF)
            hi[m * chip : (m + 1) * chip, :] = top
            lo[m * chip : (m + 1) * chip, :] = (t - top.astype(F32)).astype(BF)
    for kx in range(NX):
        part = jnp.dot(hi[...], occ[kx], preferred_element_type=F32)
        part = (part + jnp.dot(lo[...], occ[kx], preferred_element_type=F32)) * scale
        for ky in range(NY):
            near[ky, kx] = part[ky * chip : (ky + 1) * chip]
            far[kx, ky] = part[(NY + ky) * chip : (NY + ky + 1) * chip]


def gamma_occ_kernel(c, s, hi, lo, b_all, *more):
    xi = s[0]
    base, out = more if len(more) > 1 else (None, *more)
    ni, na, nq = out.shape
    nqo = nq // (NX * NZL)
    picked = [slice((2 * i + c) * na, (2 * i + c + 1) * na) for i in range(ni)]
    hi_t, lo_t = hi[...].T, lo[...].T
    hi_t = jnp.concatenate([hi_t[p] for p in picked], axis=0)
    lo_t = jnp.concatenate([lo_t[p] for p in picked], axis=0)
    for xa in range(NX):
        b = b_all[(xi - xa) & (NX - 1)]
        rows = jnp.dot(hi_t, b, preferred_element_type=F32) + jnp.dot(lo_t, b, preferred_element_type=F32)
        for i in range(ni):
            block = rows[i * na : (i + 1) * na]
            for zl in range(NZL):
                q = (zl * NX + xa) * nqo
                part = block[:, zl * nqo : (zl + 1) * nqo]
                out[i, :, q : q + nqo] = part if base is None else part + base[i, :, q : q + nqo]


def tiles_kernel(s, near, far, *outs):
    zl = s[0]
    nqo = outs[0].shape[1]
    for h, half in enumerate((near, far)):
        cols = [half[:, k * nqo : (k + 1) * nqo] for k in range(NZL)]
        for t in range(NZL):
            tile = cols[t]
            for own in range(1, NZL):
                tile = jnp.where(zl == own, cols[own ^ t], tile)
            outs[h * NZL + t][...] = tile


def ring_gather(a, b, axis):
    a1, b3 = shift(a, axis, 1, 4), shift(b, axis, 3, 4)
    b1, a3 = shift(b, axis, 1, 4), shift(a, axis, 3, 4)
    a2, b2 = shift(a1, axis, 1, 4), shift(b3, axis, 3, 4)
    return [a, b, a1, b1, a2, b2, a3, b3]


def ring_sum(blocks, axis):
    def half(k, h):
        return blocks[k, 2 * h : 2 * h + 2]

    a2, b2 = shift(half(2, 0).astype(F16), axis, 3, 4), shift(half(2, 1).astype(F16), axis, 1, 4)
    b1, a3 = shift(half(1, 1).astype(F16), axis, 3, 4), shift(half(3, 0).astype(F16), axis, 1, 4)
    a1 = shift((half(1, 0) + a2.astype(F32)).astype(F16), axis, 3, 4)
    b3 = shift((half(3, 1) + b2.astype(F32)).astype(F16), axis, 1, 4)
    return (
        half(0, 0) + a1.astype(F32) + a3.astype(F32),
        half(0, 1) + b1.astype(F32) + b3.astype(F32),
    )


def sum_direct(blocks, axis):
    total = blocks[0].astype(F32)
    for k in range(1, 4):
        total = total + shift(blocks[k], axis, 4 - k, 4).astype(F32)
    return total


def on_device(b_occ, b_outer, eps_occ, eps_outer, eps_vir):
    ni, na, nq = b_occ.shape
    nqo = b_outer.shape[2]
    core, xi, zh, y, zl = (lax.axis_index(n) for n in ("core", "x", "zh", "y", "zl"))
    wide = LANES * -(-(NZL * nqo + 2 * EXTRA) // LANES)
    chip = 2 * na
    rows, nv = ni * chip, NM * chip

    keep, give = call(
        message_kernel, [((na, nqo + EXTRA), BF)] * 2, [core], b_occ, b_outer, eps_vir.reshape(1, na)
    )
    mine = jnp.concatenate([keep, lax.ppermute(give, "core", CORES)], axis=0)

    along_z = [mine] + [swap_z(mine, t) for t in range(1, NZH * NZL)]
    near, far = call(
        lay_out_kernel, [((chip, wide), BF)] * 2, [zl], *along_z,
        scratch=[pltpu.VMEM((NZH * NZL, *mine.shape), BF)],
    )

    near_x = [near] + [shift(near, "x", k, NX) for k in range(1, NX)]
    far_y = [far] + [shift(far, "y", k, NY) for k in range(1, NY)]
    near_all = ring_gather(jnp.stack(near_x[:2]), jnp.stack(near_x[2:]), "y")
    far_all = ring_gather(jnp.stack(far_y[:2]), jnp.stack(far_y[2:]), "x")

    other_rows = lax.ppermute(b_occ, "core", CORES)
    (occ_all,) = call(occ_kernel, [((NX, rows, wide), BF)], [xi], b_occ, other_rows)

    work = 2 * rows * nv * NX * wide
    eps_here = jnp.sum(mine[:, nqo : nqo + 3].astype(F32), axis=1)
    eps_j = jnp.where(core == 0, eps_outer[0], eps_outer[1])
    eps_row = (eps_occ[:, None] + eps_j - eps_here[None, :]).reshape(rows)

    b_all, amps_t, scaled, scales = call(
        lambda *refs: amps_kernel(ni, nqo, *refs),
        [((NX, nv, wide), BF), ((nv, rows), F32), ((NM, chip, rows), F32), ((8, LANES), F32)],
        [zh, y], *near_all, *far_all, occ_all, eps_row[None, :], eps_row[:, None],
        flops=work * 2,
    )
    swapped_t = lax.all_to_all(scaled.astype(F16), ("zh", "y"), 0, 0, tiled=True).astype(F32)
    hi, lo, near_p, far_p = call(
        tilde_kernel,
        [((nv, rows), BF)] * 2 + [((NY, NX, chip, wide), F32), ((NX, NY, chip, wide), F32)],
        [zh, y], amps_t, swapped_t, occ_all, scales,
        flops=work * 2,
    )

    near_a, near_b = ring_sum(near_p, "y")
    far_a, far_b = ring_sum(far_p, "x")
    near_s = [(p[k] * 0.25).astype(F16) for p in (near_a, near_b) for k in range(2)]
    far_s = [(p[k] * 0.25).astype(F16) for p in (far_a, far_b) for k in range(2)]
    near_t, far_t = sum_direct(near_s, "x") * 0.25, sum_direct(far_s, "y") * 0.25

    (given,) = call(
        functools.partial(gamma_occ_kernel, 1), [((ni, na, nq), F32)], [xi], hi, lo, b_all, flops=work
    )
    (gamma_occ,) = call(
        functools.partial(gamma_occ_kernel, 0), [((ni, na, nq), F32)], [xi], hi, lo, b_all,
        lax.ppermute(given, "core", CORES), flops=work,
    )

    tiles = [t.astype(F16) for t in call(tiles_kernel, [((chip, nqo), F32)] * (NZH * NZL), [zl], near_t, far_t)]
    arrived = [tiles[0]] + [swap_z(tiles[t], t) for t in range(1, NZH * NZL)]
    *arrived, gamma_occ = lax.optimization_barrier((*arrived, gamma_occ))
    section = sum(t.astype(F32) for t in arrived) * (16.0 * scales[3, 0])
    mine_j, other_j = section[:na], lax.ppermute(section[na:], "core", CORES)
    gamma_outer = jnp.where(core == 0, jnp.stack([mine_j, other_j]), jnp.stack([other_j, mine_j]))
    return (gamma_occ, gamma_outer)


def solution(mesh):
    fine = Mesh(mesh.devices.reshape(SIZES), AXES)
    occ, vir = ("zl", "x"), ("zh", "y", "core")
    return jax.shard_map(
        on_device,
        mesh=fine,
        in_specs=(P(occ, vir, None), P(None, vir, occ), P(occ), P(), P(vir)),
        out_specs=(P(occ, vir, None), P(None, vir, occ)),
        check_vma=False,
    )
```

```python
import functools
import math

import jax
import jax.numpy as jnp
from jax import lax
from jax.experimental import pallas as pl
from jax.experimental.pallas import tpu as pltpu
from jax.sharding import Mesh
from jax.sharding import PartitionSpec as P


AXES = ("zl", "x", "zh", "y", "core")
SIZES = (4, 4, 2, 4, 2)
NX, NY, NZL, NZH = 4, 4, 4, 2
NM = NZH * NY
BF, F16, F32 = jnp.bfloat16, jnp.float16, jnp.float32
EXTRA = 16
OCC_TOP, OUTER_TOP = 3, 4
LANES = 128
LIMIT = 28
SMEM = pl.BlockSpec(memory_space=pltpu.SMEM)
VMEM = pl.BlockSpec(memory_space=pltpu.VMEM)
CORES = [(0, 1), (1, 0)]


def call(kernel, outs, scalars, *arrays, flops=0, scratch=()):
    moved = sum(a.size * a.dtype.itemsize for a in arrays) + sum(4 * math.prod(s) for s, _ in outs)
    return pl.pallas_call(
        kernel,
        out_shape=[jax.ShapeDtypeStruct(s, d) for s, d in outs],
        in_specs=[SMEM] + [VMEM] * len(arrays),
        out_specs=[VMEM] * len(outs),
        scratch_shapes=list(scratch),
        cost_estimate=pl.CostEstimate(flops=flops, bytes_accessed=moved, transcendentals=0),
        compiler_params=pltpu.CompilerParams(vmem_limit_bytes=LIMIT * 2**20),
    )(jnp.stack(scalars).astype(jnp.int32), *arrays)


def shift(array, axis, k, size):
    return lax.ppermute(array, axis, [(p, (p + k) % size) for p in range(size)])


def swap_z(array, t):
    flip = t % NZL * NZH + t // NZL
    return lax.ppermute(array, ("zl", "zh"), [(p, p ^ flip) for p in range(NZH * NZL)])


def nt(a, b):
    return lax.dot_general(a, b, (((1,), (1,)), ((), ())), preferred_element_type=F32)


def message_kernel(s, occ, outer, eps, keep, give):
    core = s[0]
    occ_top = jnp.max(jnp.abs(occ[...].astype(F32)))
    n = eps.shape[1]
    here = lax.broadcasted_iota(jnp.int32, (n, n), 0) == lax.broadcasted_iota(jnp.int32, (n, n), 1)
    e = jnp.sum(jnp.where(here, eps[...], 0.0), axis=1, keepdims=True)
    parts = []
    for _ in range(3):
        part = e.astype(BF).astype(F32)
        parts.append(part)
        e = e - part
    na, nqo = outer.shape[1:]
    lane = lax.broadcasted_iota(jnp.int32, (na, EXTRA), 1)
    for out, j in ((keep, core), (give, 1 - core)):
        rows = outer[j]
        row_top = jnp.max(jnp.abs(rows.astype(F32)), axis=1, keepdims=True)
        side = jnp.where(lane == OCC_TOP, occ_top, 0.0)
        for n, part in enumerate(parts):
            side = jnp.where(lane == n, part, side)
        side = jnp.where(lane == OUTER_TOP, row_top, side)
        out[:, :nqo] = rows
        out[:, nqo:] = side.astype(BF)


def groups(rows, width):
    fit = [g for g in range(LANES // width, 0, -1) if rows % g == 0]
    return next((g for g in fit if rows // g % 8 == 0), fit[0])


def packed_rows(rows, width):
    return rows + rows // groups(rows, width - LANES)


def pack(block):
    rows, few = block.shape[0], block.shape[1] - LANES
    n = groups(rows, few)
    each = rows // n
    tail = [block[g * each : (g + 1) * each, LANES:] for g in range(n)]
    if n * few < LANES:
        tail.append(jnp.zeros((each, LANES - n * few), F32))
    return jnp.concatenate([block[:, :LANES], jnp.concatenate(tail, axis=1)], axis=0)


def unpack(packed, rows, width):
    few = width - LANES
    n = groups(rows, few)
    tail = jnp.concatenate([packed[rows:, g * few : (g + 1) * few] for g in range(n)], axis=0)
    return jnp.concatenate([packed[:rows], tail], axis=1)


def pack_kernel(s, keep, got, out):
    out[...] = pack(jnp.concatenate([keep[...].astype(F32), got[...].astype(F32)], axis=0)).astype(BF)


def section_kernel(s, packed, scale, keep, give):
    na, width = keep.shape
    block = unpack(packed[...], 2 * na, width) * scale[...]
    keep[...] = block[:na]
    give[...] = block[na:]


def lay_out_kernel(nqo, s, *refs):
    zl = s[0]
    pieces, (near, far, z) = refs[: NZH * NZL], refs[NZH * NZL :]
    for t, piece in enumerate(pieces):
        z[t // NZL * NZL + (zl ^ (t % NZL))] = piece[...]
    rows, wide = near.shape
    for out, half in ((near, 0), (far, 1)):
        blocks = [unpack(z[half * NZL + k].astype(F32), rows, nqo + EXTRA) for k in range(NZL)]
        most = blocks[0][:, nqo:]
        for b in blocks[1:]:
            most = jnp.maximum(most, b[:, nqo:])
        used = NZL * nqo + 2 * EXTRA
        out[...] = jnp.concatenate(
            [b[:, :nqo] for b in blocks] + [blocks[0][:, nqo:], most, jnp.zeros((rows, wide - used), F32)], axis=1
        ).astype(BF)


def occ_kernel(s, own, other, out):
    xi = s[0]
    ni, na, nq = own.shape
    nqo, wide = nq // (NX * NZL), out.shape[2]
    for xa in range(NX):
        kx = (xi - xa) & (NX - 1)
        for i in range(ni):
            for c, src in enumerate((own, other)):
                cols = [src[i, :, (zl * NX + xa) * nqo : (zl * NX + xa + 1) * nqo] for zl in range(NZL)]
                cols.append(jnp.zeros((na, wide - NZL * nqo), BF))
                at = (2 * i + c) * na
                out[kx, at : at + na, :] = jnp.concatenate(cols, axis=1)


def amps_kernel(ni, nqo, s, *refs):
    zh, y = s[0], s[1]
    near, far, (occ, eps_lane, eps_sub, b_all, at, send, scales) = refs[:8], refs[8:16], refs[16:]
    chip = near[0].shape[1]
    half = NY * chip
    for k in range(4):
        for other in range(4):
            b_all[other, k * chip : (k + 1) * chip, :] = near[2 * k + other // 2][other % 2]
            at_row = half + other * chip
            b_all[k, at_row : at_row + chip, :] = far[2 * k + other // 2][other % 2]
    tile = NZL * nqo // LANES * LANES
    off = NZL * nqo - tile
    tail = b_all[0, :, tile : tile + LANES].astype(F32)
    eps_b_sub = tail[:, off : off + 1] + tail[:, off + 1 : off + 2] + tail[:, off + 2 : off + 3]
    lane8 = lax.broadcasted_iota(jnp.int32, (8, LANES), 1)
    pick = jnp.where((lane8 >= off) & (lane8 < off + 3), 1.0, 0.0).astype(BF)
    eps_b_lane = nt(pick, b_all[0, :, tile : tile + LANES])[0:1]
    most = jnp.max(tail, axis=0, keepdims=True)
    for kx in range(1, NX):
        most = jnp.maximum(most, jnp.max(b_all[kx, :, tile : tile + LANES].astype(F32), axis=0, keepdims=True))
    lane1 = lax.broadcasted_iota(jnp.int32, (1, LANES), 1)

    def extra(n):
        return jnp.sum(jnp.where(lane1 == off + EXTRA + n, most, 0.0), axis=1, keepdims=True)

    nq = NX * NZL * nqo
    amp_top = jnp.maximum(nq * extra(OCC_TOP) * extra(OUTER_TOP), 1e-30)
    sum_top = jnp.maximum(3.0 * ni * chip * amp_top * extra(OCC_TOP), 1e-30)
    amp_scale, sum_scale = 60000.0 / amp_top, 15000.0 / sum_top
    for n, value in enumerate((amp_scale, amp_top / 60000.0, sum_scale, sum_top / 15000.0)):
        scales[n : n + 1, :] = jnp.broadcast_to(value, (1, LANES))

    total = nt(occ[0], b_all[0])
    total_t = nt(b_all[0], occ[0])
    for kx in range(1, NX):
        total = total + nt(occ[kx], b_all[kx])
        total_t = total_t + nt(b_all[kx], occ[kx])
    at[...] = total_t / (eps_lane[...] - eps_b_sub)
    scaled = total / (eps_sub[...] - eps_b_lane) * amp_scale
    for h in range(NZH):
        for k in range(NY):
            m, to = h * NY + k, (zh ^ h) * NY + ((y - k) & (NY - 1))
            send[to] = jnp.concatenate(
                [scaled[i * chip : (i + 1) * chip, m * chip : (m + 1) * chip] for i in range(ni)], axis=1
            )


def tilde_kernel(s, at, st, occ, scales, hi, lo, near, far):
    zh, y = s[0], s[1]
    chip = st.shape[1]
    back, scale = scales[1:2, 0:1], scales[2:3, 0:1]
    for h in range(NZH):
        for k in range(NY):
            m, to = h * NY + k, (zh ^ h) * NY + ((y - k) & (NY - 1))
            t = 2.0 * at[m * chip : (m + 1) * chip, :] - st[to] * back
            top = t.astype(BF)
            hi[m * chip : (m + 1) * chip, :] = top
            lo[m * chip : (m + 1) * chip, :] = (t - top.astype(F32)).astype(BF)
    for kx in range(NX):
        part = jnp.dot(hi[...], occ[kx], preferred_element_type=F32)
        part = (part + jnp.dot(lo[...], occ[kx], preferred_element_type=F32)) * scale
        for ky in range(NY):
            near[ky, kx] = part[ky * chip : (ky + 1) * chip]
            far[kx, ky] = part[(NY + ky) * chip : (NY + ky + 1) * chip]


def gamma_occ_kernel(c, s, hi, lo, b_all, *more):
    xi = s[0]
    base, out = more if len(more) > 1 else (None, *more)
    ni, na, nq = out.shape
    nqo = nq // (NX * NZL)
    picked = [slice((2 * i + c) * na, (2 * i + c + 1) * na) for i in range(ni)]
    hi_t, lo_t = hi[...].T, lo[...].T
    hi_t = jnp.concatenate([hi_t[p] for p in picked], axis=0)
    lo_t = jnp.concatenate([lo_t[p] for p in picked], axis=0)
    for xa in range(NX):
        b = b_all[(xi - xa) & (NX - 1)]
        rows = jnp.dot(hi_t, b, preferred_element_type=F32) + jnp.dot(lo_t, b, preferred_element_type=F32)
        for i in range(ni):
            block = rows[i * na : (i + 1) * na]
            for zl in range(NZL):
                q = (zl * NX + xa) * nqo
                part = block[:, zl * nqo : (zl + 1) * nqo]
                out[i, :, q : q + nqo] = part if base is None else part + base[i, :, q : q + nqo]


def tiles_kernel(nqo, s, near, far, *outs):
    zl = s[0]
    for h, half in enumerate((near, far)):
        cols = [half[:, k * nqo : (k + 1) * nqo] for k in range(NZL)]
        for t in range(NZL):
            tile = cols[t]
            for own in range(1, NZL):
                tile = jnp.where(zl == own, cols[own ^ t], tile)
            outs[h * NZL + t][...] = pack(tile)


def ring_gather(a, b, axis):
    a1, b3 = shift(a, axis, 1, 4), shift(b, axis, 3, 4)
    b1, a3 = shift(b, axis, 1, 4), shift(a, axis, 3, 4)
    a2, b2 = shift(a1, axis, 1, 4), shift(b3, axis, 3, 4)
    return [a, b, a1, b1, a2, b2, a3, b3]


def ring_sum(blocks, axis):
    def half(k, h):
        return blocks[k, 2 * h : 2 * h + 2]

    a2, b2 = shift(half(2, 0).astype(F16), axis, 3, 4), shift(half(2, 1).astype(F16), axis, 1, 4)
    b1, a3 = shift(half(1, 1).astype(F16), axis, 3, 4), shift(half(3, 0).astype(F16), axis, 1, 4)
    a1 = shift((half(1, 0) + a2.astype(F32)).astype(F16), axis, 3, 4)
    b3 = shift((half(3, 1) + b2.astype(F32)).astype(F16), axis, 1, 4)
    return (
        half(0, 0) + a1.astype(F32) + a3.astype(F32),
        half(0, 1) + b1.astype(F32) + b3.astype(F32),
    )


def sum_direct(blocks, axis):
    total = blocks[0].astype(F32)
    for k in (1, 3, 2):
        total = total + shift(blocks[k], axis, 4 - k, 4).astype(F32)
    return total


def whole(b_occ, b_outer, eps_occ, eps_outer, eps_vir):
    ni, na, nq = b_occ.shape
    nqo = b_outer.shape[2]
    core, xi, zh, y, zl = (lax.axis_index(n) for n in ("core", "x", "zh", "y", "zl"))
    wide = LANES * -(-(NZL * nqo + 2 * EXTRA) // LANES)
    chip = 2 * na
    rows, nv = ni * chip, NM * chip

    keep, give = call(
        message_kernel, [((na, nqo + EXTRA), BF)] * 2, [core], b_occ, b_outer, eps_vir.reshape(1, na)
    )
    got = lax.ppermute(give, "core", CORES)
    few = packed_rows(chip, nqo + EXTRA)
    (mine,) = call(pack_kernel, [((few, LANES), BF)], [core], keep, got)

    along_z = [mine] + [swap_z(mine, t) for t in range(1, NZH * NZL)]
    near, far = call(
        functools.partial(lay_out_kernel, nqo), [((chip, wide), BF)] * 2, [zl], *along_z,
        scratch=[pltpu.VMEM((NZH * NZL, *mine.shape), BF)],
    )

    near_x = [near] + [shift(near, "x", k, NX) for k in range(1, NX)]
    far_y = [far] + [shift(far, "y", k, NY) for k in range(1, NY)]
    near_all = ring_gather(jnp.stack(near_x[:2]), jnp.stack(near_x[2:]), "y")
    far_all = ring_gather(jnp.stack(far_y[:2]), jnp.stack(far_y[2:]), "x")

    other_rows = lax.ppermute(b_occ, "core", CORES)
    (occ_all,) = call(occ_kernel, [((NX, rows, wide), BF)], [xi], b_occ, other_rows)

    work = 2 * rows * nv * NX * wide
    eps_here = jnp.concatenate([eps_vir, jnp.sum(got[:, nqo : nqo + 3].astype(F32), axis=1)])
    eps_j = jnp.where(core == 0, eps_outer[0], eps_outer[1])
    eps_row = (eps_occ[:, None] + eps_j - eps_here[None, :]).reshape(rows)

    b_all, amps_t, scaled, scales = call(
        lambda *refs: amps_kernel(ni, nqo, *refs),
        [((NX, nv, wide), BF), ((nv, rows), F32), ((NM, chip, rows), F32), ((8, LANES), F32)],
        [zh, y], *near_all, *far_all, occ_all, eps_row[None, :], eps_row[:, None],
        flops=work * 2,
    )
    swapped_t = lax.all_to_all(scaled.astype(F16), ("zh", "y"), 0, 0, tiled=True).astype(F32)
    hi, lo, near_p, far_p = call(
        tilde_kernel,
        [((nv, rows), BF)] * 2 + [((NY, NX, chip, wide), F32), ((NX, NY, chip, wide), F32)],
        [zh, y], amps_t, swapped_t, occ_all, scales,
        flops=work * 2,
    )

    near_a, near_b = ring_sum(near_p, "y")
    far_a, far_b = ring_sum(far_p, "x")
    near_s = [(p[k] * 0.25).astype(F16) for p in (near_a, near_b) for k in range(2)]
    far_s = [(p[k] * 0.25).astype(F16) for p in (far_a, far_b) for k in range(2)]
    near_t, far_t = sum_direct(near_s, "x") * 0.25, sum_direct(far_s, "y") * 0.25

    (given,) = call(
        functools.partial(gamma_occ_kernel, 1), [((ni, na, nq), F32)], [xi], hi, lo, b_all, flops=work
    )
    given = lax.ppermute(given, "core", CORES)
    (gamma_occ,) = call(
        functools.partial(gamma_occ_kernel, 0), [((ni, na, nq), F32)], [xi], hi, lo, b_all, given, flops=work
    )

    small = (packed_rows(chip, nqo), LANES)
    tiles = call(functools.partial(tiles_kernel, nqo), [(small, F32)] * (NZH * NZL), [zl], near_t, far_t)
    tiles = [t.astype(F16) for t in tiles]
    arrived = [tiles[0]] + [swap_z(tiles[t], t) for t in range(1, NZH * NZL)]
    mine_j, give_j = call(
        section_kernel, [((na, nqo), F32)] * 2, [core],
        sum(t.astype(F32) for t in arrived), 16.0 * scales[3:4, 0:1],
    )
    other_j = lax.ppermute(give_j, "core", CORES)
    gamma_outer = jnp.where(core == 0, jnp.stack([mine_j, other_j]), jnp.stack([other_j, mine_j]))
    return (gamma_occ, gamma_outer)


def solution(mesh):
    fine = Mesh(mesh.devices.reshape(SIZES), AXES)
    occ, vir = ("zl", "x"), ("zh", "y", "core")
    return jax.shard_map(
        whole,
        mesh=fine,
        in_specs=(P(occ, vir, None), P(None, vir, occ), P(occ), P(), P(vir)),
        out_specs=(P(occ, vir, None), P(None, vir, occ)),
        check_vma=False,
    )
```

```python
import functools
import math

import jax
import jax.numpy as jnp
from jax import lax
from jax.experimental import pallas as pl
from jax.experimental.pallas import tpu as pltpu
from jax.sharding import Mesh
from jax.sharding import PartitionSpec as P


AXES = ("zl", "x", "zh", "y", "core")
SIZES = (4, 4, 2, 4, 2)
NX, NY, NZL, NZH = 4, 4, 4, 2
NM = NZH * NY
BF, F16, F32 = jnp.bfloat16, jnp.float16, jnp.float32
EXTRA = 16
OCC_TOP, OUTER_TOP = 3, 4
LANES = 128
LIMIT = 28
SMEM = pl.BlockSpec(memory_space=pltpu.SMEM)
VMEM = pl.BlockSpec(memory_space=pltpu.VMEM)
CORES = [(0, 1), (1, 0)]


def call(kernel, outs, scalars, *arrays, flops=0, scratch=()):
    moved = sum(a.size * a.dtype.itemsize for a in arrays) + sum(4 * math.prod(s) for s, _ in outs)
    return pl.pallas_call(
        kernel,
        out_shape=[jax.ShapeDtypeStruct(s, d) for s, d in outs],
        in_specs=[SMEM] + [VMEM] * len(arrays),
        out_specs=[VMEM] * len(outs),
        scratch_shapes=list(scratch),
        cost_estimate=pl.CostEstimate(flops=flops, bytes_accessed=moved, transcendentals=0),
        compiler_params=pltpu.CompilerParams(vmem_limit_bytes=LIMIT * 2**20),
    )(jnp.stack(scalars).astype(jnp.int32), *arrays)


def shift(array, axis, k, size):
    return lax.ppermute(array, axis, [(p, (p + k) % size) for p in range(size)])


def shift_z(array, k):
    def place(z):
        return z % NZL * NZH + z // NZL

    size = NZH * NZL
    return lax.ppermute(array, ("zl", "zh"), [(place(z), place((z + k) % size)) for z in range(size)])


def nt(a, b):
    return lax.dot_general(a, b, (((1,), (1,)), ((), ())), preferred_element_type=F32)


def message_kernel(s, occ, outer, eps, keep, give):
    core = s[0]
    occ_top = jnp.max(jnp.abs(occ[...].astype(F32)))
    n = eps.shape[1]
    here = lax.broadcasted_iota(jnp.int32, (n, n), 0) == lax.broadcasted_iota(jnp.int32, (n, n), 1)
    e = jnp.sum(jnp.where(here, eps[...], 0.0), axis=1, keepdims=True)
    parts = []
    for _ in range(3):
        part = e.astype(BF).astype(F32)
        parts.append(part)
        e = e - part
    na, nqo = outer.shape[1:]
    lane = lax.broadcasted_iota(jnp.int32, (na, EXTRA), 1)
    for out, j in ((keep, core), (give, 1 - core)):
        rows = outer[j]
        row_top = jnp.max(jnp.abs(rows.astype(F32)), axis=1, keepdims=True)
        side = jnp.where(lane == OCC_TOP, occ_top, 0.0)
        for n, part in enumerate(parts):
            side = jnp.where(lane == n, part, side)
        side = jnp.where(lane == OUTER_TOP, row_top, side)
        out[:, :nqo] = rows
        out[:, nqo:] = side.astype(BF)


def groups(rows, width):
    fit = [g for g in range(LANES // width, 0, -1) if rows % g == 0]
    return next((g for g in fit if rows // g % 8 == 0), fit[0])


def packed_rows(rows, width):
    return rows + rows // groups(rows, width - LANES)


def pack(block):
    rows, few = block.shape[0], block.shape[1] - LANES
    n = groups(rows, few)
    each = rows // n
    tail = [block[g * each : (g + 1) * each, LANES:] for g in range(n)]
    if n * few < LANES:
        tail.append(jnp.zeros((each, LANES - n * few), F32))
    return jnp.concatenate([block[:, :LANES], jnp.concatenate(tail, axis=1)], axis=0)


def unpack(packed, rows, width):
    few = width - LANES
    n = groups(rows, few)
    tail = jnp.concatenate([packed[rows:, g * few : (g + 1) * few] for g in range(n)], axis=0)
    return jnp.concatenate([packed[:rows], tail], axis=1)


def pack_kernel(s, keep, got, out):
    out[...] = pack(jnp.concatenate([keep[...].astype(F32), got[...].astype(F32)], axis=0)).astype(BF)


def section_kernel(s, own, up, down, scales, keep, give):
    na, width = keep.shape
    packed = (own[...] + up[...] + down[...]) * (16.0 * scales[3:4, 0:1])
    block = unpack(packed, 2 * na, width)
    keep[...] = block[:na]
    give[...] = block[na:]


def lay_out_kernel(nqo, s, *refs):
    zl = s[0]
    pieces, (near, far, z) = refs[: NZH * NZL], refs[NZH * NZL :]
    for d, piece in enumerate(pieces):
        z[(zl - d) & (NZH * NZL - 1)] = piece[...]
    rows, wide = near.shape
    for out, half in ((near, 0), (far, 1)):
        blocks = [unpack(z[half * NZL + k].astype(F32), rows, nqo + EXTRA) for k in range(NZL)]
        most = blocks[0][:, nqo:]
        for b in blocks[1:]:
            most = jnp.maximum(most, b[:, nqo:])
        used = NZL * nqo + 2 * EXTRA
        out[...] = jnp.concatenate(
            [b[:, :nqo] for b in blocks] + [blocks[0][:, nqo:], most, jnp.zeros((rows, wide - used), F32)], axis=1
        ).astype(BF)


def occ_kernel(s, own, other, out):
    xi = s[0]
    ni, na, nq = own.shape
    nqo, wide = nq // (NX * NZL), out.shape[2]
    for xa in range(NX):
        kx = (xi - xa) & (NX - 1)
        for i in range(ni):
            for c, src in enumerate((own, other)):
                cols = [src[i, :, (zl * NX + xa) * nqo : (zl * NX + xa + 1) * nqo] for zl in range(NZL)]
                cols.append(jnp.zeros((na, wide - NZL * nqo), BF))
                at = (2 * i + c) * na
                out[kx, at : at + na, :] = jnp.concatenate(cols, axis=1)


def amps_kernel(ni, nqo, s, *refs):
    zh, y = s[0], s[1]
    near, far, (occ, eps_lane, eps_sub, eps_outer, b_all, at, send, scales) = refs[:8], refs[8:16], refs[16:]
    chip = near[0].shape[1]
    half = NY * chip
    for k in range(4):
        for other in range(4):
            b_all[other, k * chip : (k + 1) * chip, :] = near[2 * k + other // 2][other % 2]
            at_row = half + other * chip
            b_all[k, at_row : at_row + chip, :] = far[2 * k + other // 2][other % 2]
    tile = NZL * nqo // LANES * LANES
    off = NZL * nqo - tile
    tail = b_all[0, :, tile : tile + LANES].astype(F32)
    eps_b_sub = tail[:, off : off + 1] + tail[:, off + 1 : off + 2] + tail[:, off + 2 : off + 3]
    lane8 = lax.broadcasted_iota(jnp.int32, (8, LANES), 1)
    pick = jnp.where((lane8 >= off) & (lane8 < off + 3), 1.0, 0.0).astype(BF)
    eps_b_lane = nt(pick, b_all[0, :, tile : tile + LANES])[0:1]
    most = jnp.max(tail, axis=0, keepdims=True)
    for kx in range(1, NX):
        most = jnp.maximum(most, jnp.max(b_all[kx, :, tile : tile + LANES].astype(F32), axis=0, keepdims=True))
    lane1 = lax.broadcasted_iota(jnp.int32, (1, LANES), 1)

    def extra(n):
        return jnp.sum(jnp.where(lane1 == off + EXTRA + n, most, 0.0), axis=1, keepdims=True)

    nq = NX * NZL * nqo
    amp_top = jnp.maximum(nq * extra(OCC_TOP) * extra(OUTER_TOP), 1e-30)
    sum_top = jnp.maximum(3.0 * ni * chip * amp_top * extra(OCC_TOP), 1e-30)
    amp_scale, sum_scale = 60000.0 / amp_top, 15000.0 / sum_top
    for n, value in enumerate((amp_scale, amp_top / 60000.0, sum_scale, sum_top / 15000.0)):
        scales[n : n + 1, :] = jnp.broadcast_to(value, (1, LANES))

    total = nt(occ[0], b_all[0])
    total_t = nt(b_all[0], occ[0])
    for kx in range(1, NX):
        total = total + nt(occ[kx], b_all[kx])
        total_t = total_t + nt(b_all[kx], occ[kx])
    eps_j = jnp.where(s[2] == 0, eps_outer[0:1, 0:1], eps_outer[0:1, 1:2])
    at[...] = total_t / (eps_lane[...] + eps_j - eps_b_sub)
    scaled = total / (eps_sub[...] + eps_j - eps_b_lane) * amp_scale
    for h in range(NZH):
        for k in range(NY):
            m, to = h * NY + k, (zh ^ h) * NY + ((y - k) & (NY - 1))
            send[to] = jnp.concatenate(
                [scaled[i * chip : (i + 1) * chip, m * chip : (m + 1) * chip] for i in range(ni)], axis=1
            )


def tilde_kernel(s, at, st, occ, scales, hi, lo, near, far):
    zh, y = s[0], s[1]
    chip = st.shape[1]
    back, scale = scales[1:2, 0:1], scales[2:3, 0:1]
    for h in range(NZH):
        for k in range(NY):
            m, to = h * NY + k, (zh ^ h) * NY + ((y - k) & (NY - 1))
            t = 2.0 * at[m * chip : (m + 1) * chip, :] - st[to] * back
            top = t.astype(BF)
            hi[m * chip : (m + 1) * chip, :] = top
            lo[m * chip : (m + 1) * chip, :] = (t - top.astype(F32)).astype(BF)
    for kx in range(NX):
        part = jnp.dot(hi[...], occ[kx], preferred_element_type=F32)
        part = (part + jnp.dot(lo[...], occ[kx], preferred_element_type=F32)) * scale
        for ky in range(NY):
            near[ky, kx] = part[ky * chip : (ky + 1) * chip]
            far[kx, ky] = part[(NY + ky) * chip : (NY + ky + 1) * chip]


def gamma_occ_kernel(c, s, hi, lo, b_all, *more):
    xi = s[0]
    base, out = more if len(more) > 1 else (None, *more)
    ni, na, nq = out.shape
    nqo = nq // (NX * NZL)
    picked = [slice((2 * i + c) * na, (2 * i + c + 1) * na) for i in range(ni)]
    hi_t, lo_t = hi[...].T, lo[...].T
    hi_t = jnp.concatenate([hi_t[p] for p in picked], axis=0)
    lo_t = jnp.concatenate([lo_t[p] for p in picked], axis=0)
    for xa in range(NX):
        b = b_all[(xi - xa) & (NX - 1)]
        rows = jnp.dot(hi_t, b, preferred_element_type=F32) + jnp.dot(lo_t, b, preferred_element_type=F32)
        for i in range(ni):
            block = rows[i * na : (i + 1) * na]
            for zl in range(NZL):
                q = (zl * NX + xa) * nqo
                part = block[:, zl * nqo : (zl + 1) * nqo]
                out[i, :, q : q + nqo] = part if base is None else part + base[i, :, q : q + nqo]


def tiles_kernel(nqo, s, near, far, *outs):
    zl = s[0]
    cols = [half[:, k * nqo : (k + 1) * nqo] for half in (near, far) for k in range(NZL)]
    for e, out in enumerate(outs):
        tile = cols[e]
        for own in range(1, NZL):
            tile = jnp.where(zl == own, cols[(e + own) % len(cols)], tile)
        out[...] = pack(tile)


def ring_gather(a, b, axis):
    a1, b3 = shift(a, axis, 1, 4), shift(b, axis, 3, 4)
    b1, a3 = shift(b, axis, 1, 4), shift(a, axis, 3, 4)
    a2, b2 = shift(a1, axis, 1, 4), shift(b3, axis, 3, 4)
    return [a, b, a1, b1, a2, b2, a3, b3]


def ring_sum(blocks, axis):
    def half(k, h):
        return blocks[k, 2 * h : 2 * h + 2]

    a2, b2 = shift(half(2, 0).astype(F16), axis, 3, 4), shift(half(2, 1).astype(F16), axis, 1, 4)
    b1, a3 = shift(half(1, 1).astype(F16), axis, 3, 4), shift(half(3, 0).astype(F16), axis, 1, 4)
    a1 = shift((half(1, 0) + a2.astype(F32)).astype(F16), axis, 3, 4)
    b3 = shift((half(3, 1) + b2.astype(F32)).astype(F16), axis, 1, 4)
    return (
        half(0, 0) + a1.astype(F32) + a3.astype(F32),
        half(0, 1) + b1.astype(F32) + b3.astype(F32),
    )


def sum_direct(blocks, axis):
    total = blocks[0].astype(F32)
    for k in (1, 3, 2):
        total = total + shift(blocks[k], axis, 4 - k, 4).astype(F32)
    return total


def whole(b_occ, b_outer, eps_occ, eps_outer, eps_vir):
    ni, na, nq = b_occ.shape
    nqo = b_outer.shape[2]
    core, xi, zh, y, zl = (lax.axis_index(n) for n in ("core", "x", "zh", "y", "zl"))
    wide = LANES * -(-(NZL * nqo + 2 * EXTRA) // LANES)
    chip = 2 * na
    rows, nv = ni * chip, NM * chip

    keep, give = call(
        message_kernel, [((na, nqo + EXTRA), BF)] * 2, [core], b_occ, b_outer, eps_vir.reshape(1, na)
    )
    got = lax.ppermute(give, "core", CORES)
    few = packed_rows(chip, nqo + EXTRA)
    (mine,) = call(pack_kernel, [((few, LANES), BF)], [core], keep, got)

    ahead, behind = [mine], [mine]
    for step in range(4):
        behind.append(shift_z(behind[-1], 1))
        if step < 3:
            ahead.append(shift_z(ahead[-1], -1))
    along_z = behind + ahead[:0:-1]
    near, far = call(
        functools.partial(lay_out_kernel, nqo), [((chip, wide), BF)] * 2, [zl], *along_z,
        scratch=[pltpu.VMEM((NZH * NZL, *mine.shape), BF)],
    )

    near_x = [near] + [shift(near, "x", k, NX) for k in range(1, NX)]
    far_y = [far] + [shift(far, "y", k, NY) for k in range(1, NY)]
    near_all = ring_gather(jnp.stack(near_x[:2]), jnp.stack(near_x[2:]), "y")
    far_all = ring_gather(jnp.stack(far_y[:2]), jnp.stack(far_y[2:]), "x")

    other_rows = lax.ppermute(b_occ, "core", CORES)
    (occ_all,) = call(occ_kernel, [((NX, rows, wide), BF)], [xi], b_occ, other_rows)

    work = 2 * rows * nv * NX * wide
    eps_here = jnp.concatenate([eps_vir, jnp.sum(got[:, nqo : nqo + 3].astype(F32), axis=1)])
    eps_row = (eps_occ[:, None] - eps_here[None, :]).reshape(rows)

    b_all, amps_t, scaled, scales = call(
        lambda *refs: amps_kernel(ni, nqo, *refs),
        [((NX, nv, wide), BF), ((nv, rows), F32), ((NM, chip, rows), F32), ((8, LANES), F32)],
        [zh, y, core], *near_all, *far_all, occ_all, eps_row[None, :], eps_row[:, None], eps_outer[None, :],
        flops=work * 2,
    )
    swapped_t = lax.all_to_all(scaled.astype(F16), ("zh", "y"), 0, 0, tiled=True).astype(F32)
    hi, lo, near_p, far_p = call(
        tilde_kernel,
        [((nv, rows), BF)] * 2 + [((NY, NX, chip, wide), F32), ((NX, NY, chip, wide), F32)],
        [zh, y], amps_t, swapped_t, occ_all, scales,
        flops=work * 2,
    )

    near_a, near_b = ring_sum(near_p, "y")
    far_a, far_b = ring_sum(far_p, "x")
    near_s = [(p[k] * 0.25).astype(F16) for p in (near_a, near_b) for k in range(2)]
    far_s = [(p[k] * 0.25).astype(F16) for p in (far_a, far_b) for k in range(2)]
    near_t, far_t = sum_direct(near_s, "x") * 0.25, sum_direct(far_s, "y") * 0.25

    (given,) = call(
        functools.partial(gamma_occ_kernel, 1), [((ni, na, nq), F32)], [xi], hi, lo, b_all, flops=work
    )
    given = lax.ppermute(given, "core", CORES)
    (gamma_occ,) = call(
        functools.partial(gamma_occ_kernel, 0), [((ni, na, nq), F32)], [xi], hi, lo, b_all, given, flops=work
    )

    small = (packed_rows(chip, nqo), LANES)
    tiles = call(functools.partial(tiles_kernel, nqo), [(small, F32)] * (NZH * NZL), [zl], near_t, far_t)
    up, down = tiles[4], tiles[5]
    for step in range(3):
        up = shift_z(up.astype(F16), 1).astype(F32) + tiles[3 - step]
        if step < 2:
            down = shift_z(down.astype(F16), -1).astype(F32) + tiles[6 + step]
    last = (shift_z(up.astype(F16), 1), shift_z(down.astype(F16), -1))
    mine_j, give_j = call(section_kernel, [((na, nqo), F32)] * 2, [core], tiles[0], *(t.astype(F32) for t in last), scales)
    other_j = lax.ppermute(give_j, "core", CORES)
    gamma_outer = jnp.where(core == 0, jnp.stack([mine_j, other_j]), jnp.stack([other_j, mine_j]))
    return (gamma_occ, gamma_outer)


def solution(mesh):
    fine = Mesh(mesh.devices.reshape(SIZES), AXES)
    occ, vir = ("zl", "x"), ("zh", "y", "core")
    return jax.shard_map(
        whole,
        mesh=fine,
        in_specs=(P(occ, vir, None), P(None, vir, occ), P(occ), P(), P(vir)),
        out_specs=(P(occ, vir, None), P(None, vir, occ)),
        check_vma=False,
    )
```

```python
import functools
import math

import jax
import jax.numpy as jnp
from jax import lax
from jax.experimental import pallas as pl
from jax.experimental.pallas import tpu as pltpu
from jax.sharding import Mesh
from jax.sharding import PartitionSpec as P


AXES = ("zl", "x", "zh", "y", "core")
SIZES = (4, 4, 2, 4, 2)
NX, NY, NZL, NZH = 4, 4, 4, 2
NM = NZH * NY
BF, F16, F32 = jnp.bfloat16, jnp.float16, jnp.float32
EXTRA = 16
OCC_TOP, OUTER_TOP = 3, 4
LANES = 128
LIMIT = 28
SMEM = pl.BlockSpec(memory_space=pltpu.SMEM)
VMEM = pl.BlockSpec(memory_space=pltpu.VMEM)
CORES = [(0, 1), (1, 0)]


def call(kernel, outs, scalars, *arrays, flops=0, scratch=()):
    moved = sum(a.size * a.dtype.itemsize for a in arrays) + sum(4 * math.prod(s) for s, _ in outs)
    return pl.pallas_call(
        kernel,
        out_shape=[jax.ShapeDtypeStruct(s, d) for s, d in outs],
        in_specs=[SMEM] + [VMEM] * len(arrays),
        out_specs=[VMEM] * len(outs),
        scratch_shapes=list(scratch),
        cost_estimate=pl.CostEstimate(flops=flops, bytes_accessed=moved, transcendentals=0),
        compiler_params=pltpu.CompilerParams(vmem_limit_bytes=LIMIT * 2**20),
    )(jnp.stack(scalars).astype(jnp.int32), *arrays)


def shift(array, axis, k, size):
    return lax.ppermute(array, axis, [(p, (p + k) % size) for p in range(size)])


def exchange_z(array):
    return lax.all_to_all(array, ("zh", "zl"), 0, 0, tiled=True)


def nt(a, b):
    return lax.dot_general(a, b, (((1,), (1,)), ((), ())), preferred_element_type=F32)


def message_kernel(s, occ, outer, eps, keep, give):
    core = s[0]
    occ_top = jnp.max(jnp.abs(occ[...].astype(F32)))
    n = eps.shape[1]
    here = lax.broadcasted_iota(jnp.int32, (n, n), 0) == lax.broadcasted_iota(jnp.int32, (n, n), 1)
    e = jnp.sum(jnp.where(here, eps[...], 0.0), axis=1, keepdims=True)
    parts = []
    for _ in range(3):
        part = e.astype(BF).astype(F32)
        parts.append(part)
        e = e - part
    na, nqo = outer.shape[1:]
    lane = lax.broadcasted_iota(jnp.int32, (na, EXTRA), 1)
    for out, j in ((keep, core), (give, 1 - core)):
        rows = outer[j]
        row_top = jnp.max(jnp.abs(rows.astype(F32)), axis=1, keepdims=True)
        side = jnp.where(lane == OCC_TOP, occ_top, 0.0)
        for n, part in enumerate(parts):
            side = jnp.where(lane == n, part, side)
        side = jnp.where(lane == OUTER_TOP, row_top, side)
        out[:, :nqo] = rows
        out[:, nqo:] = side.astype(BF)


def groups(rows, width):
    fit = [g for g in range(LANES // width, 0, -1) if rows % g == 0]
    return next((g for g in fit if rows // g % 8 == 0), fit[0])


def packed_rows(rows, width):
    return rows + rows // groups(rows, width - LANES)


def pack(block):
    rows, few = block.shape[0], block.shape[1] - LANES
    n = groups(rows, few)
    each = rows // n
    tail = [block[g * each : (g + 1) * each, LANES:] for g in range(n)]
    if n * few < LANES:
        tail.append(jnp.zeros((each, LANES - n * few), F32))
    return jnp.concatenate([block[:, :LANES], jnp.concatenate(tail, axis=1)], axis=0)


def unpack(packed, rows, width):
    few = width - LANES
    n = groups(rows, few)
    tail = jnp.concatenate([packed[rows:, g * few : (g + 1) * few] for g in range(n)], axis=0)
    return jnp.concatenate([packed[:rows], tail], axis=1)


def pack_kernel(s, keep, got, out):
    block = pack(jnp.concatenate([keep[...].astype(F32), got[...].astype(F32)], axis=0)).astype(BF)
    for p in range(out.shape[0]):
        out[p] = block


def section_kernel(s, packed, scales, keep, give):
    na, width = keep.shape
    block = unpack(packed[...] * (16.0 * scales[3:4, 0:1]), 2 * na, width)
    keep[...] = block[:na]
    give[...] = block[na:]


def lay_out_kernel(nqo, s, z, near, far):
    zh = s[0]
    rows, wide = near.shape
    for out, half in ((near, zh), (far, 1 - zh)):
        blocks = [unpack(z[half * NZL + k].astype(F32), rows, nqo + EXTRA) for k in range(NZL)]
        most = blocks[0][:, nqo:]
        for b in blocks[1:]:
            most = jnp.maximum(most, b[:, nqo:])
        used = NZL * nqo + 2 * EXTRA
        out[...] = jnp.concatenate(
            [b[:, :nqo] for b in blocks] + [blocks[0][:, nqo:], most, jnp.zeros((rows, wide - used), F32)], axis=1
        ).astype(BF)


def occ_kernel(s, own, other, out):
    xi = s[0]
    ni, na, nq = own.shape
    nqo, wide = nq // (NX * NZL), out.shape[2]
    for xa in range(NX):
        kx = (xi - xa) & (NX - 1)
        for i in range(ni):
            for c, src in enumerate((own, other)):
                cols = [src[i, :, (zl * NX + xa) * nqo : (zl * NX + xa + 1) * nqo] for zl in range(NZL)]
                cols.append(jnp.zeros((na, wide - NZL * nqo), BF))
                at = (2 * i + c) * na
                out[kx, at : at + na, :] = jnp.concatenate(cols, axis=1)


def amps_kernel(ni, nqo, s, *refs):
    zh, y = s[0], s[1]
    near, far, (occ, eps_lane, eps_sub, eps_outer, b_all, at, send, scales) = refs[:8], refs[8:16], refs[16:]
    chip = near[0].shape[1]
    half = NY * chip
    for k in range(4):
        for other in range(4):
            b_all[other, k * chip : (k + 1) * chip, :] = near[2 * k + other // 2][other % 2]
            at_row = half + other * chip
            b_all[k, at_row : at_row + chip, :] = far[2 * k + other // 2][other % 2]
    tile = NZL * nqo // LANES * LANES
    off = NZL * nqo - tile
    tail = b_all[0, :, tile : tile + LANES].astype(F32)
    eps_b_sub = tail[:, off : off + 1] + tail[:, off + 1 : off + 2] + tail[:, off + 2 : off + 3]
    lane8 = lax.broadcasted_iota(jnp.int32, (8, LANES), 1)
    pick = jnp.where((lane8 >= off) & (lane8 < off + 3), 1.0, 0.0).astype(BF)
    eps_b_lane = nt(pick, b_all[0, :, tile : tile + LANES])[0:1]
    most = jnp.max(tail, axis=0, keepdims=True)
    for kx in range(1, NX):
        most = jnp.maximum(most, jnp.max(b_all[kx, :, tile : tile + LANES].astype(F32), axis=0, keepdims=True))
    lane1 = lax.broadcasted_iota(jnp.int32, (1, LANES), 1)

    def extra(n):
        return jnp.sum(jnp.where(lane1 == off + EXTRA + n, most, 0.0), axis=1, keepdims=True)

    nq = NX * NZL * nqo
    amp_top = jnp.maximum(nq * extra(OCC_TOP) * extra(OUTER_TOP), 1e-30)
    sum_top = jnp.maximum(3.0 * ni * chip * amp_top * extra(OCC_TOP), 1e-30)
    amp_scale, sum_scale = 60000.0 / amp_top, 15000.0 / sum_top
    for n, value in enumerate((amp_scale, amp_top / 60000.0, sum_scale, sum_top / 15000.0)):
        scales[n : n + 1, :] = jnp.broadcast_to(value, (1, LANES))

    total = nt(occ[0], b_all[0])
    total_t = nt(b_all[0], occ[0])
    for kx in range(1, NX):
        total = total + nt(occ[kx], b_all[kx])
        total_t = total_t + nt(b_all[kx], occ[kx])
    eps_j = jnp.where(s[2] == 0, eps_outer[0:1, 0:1], eps_outer[0:1, 1:2])
    at[...] = total_t / (eps_lane[...] + eps_j - eps_b_sub)
    scaled = total / (eps_sub[...] + eps_j - eps_b_lane) * amp_scale
    for h in range(NZH):
        for k in range(NY):
            m, to = h * NY + k, (zh ^ h) * NY + ((y - k) & (NY - 1))
            send[to] = jnp.concatenate(
                [scaled[i * chip : (i + 1) * chip, m * chip : (m + 1) * chip] for i in range(ni)], axis=1
            )


def tilde_kernel(s, at, st, occ, scales, hi, lo, near, far):
    zh, y = s[0], s[1]
    chip = st.shape[1]
    back, scale = scales[1:2, 0:1], scales[2:3, 0:1]
    for h in range(NZH):
        for k in range(NY):
            m, to = h * NY + k, (zh ^ h) * NY + ((y - k) & (NY - 1))
            t = 2.0 * at[m * chip : (m + 1) * chip, :] - st[to] * back
            top = t.astype(BF)
            hi[m * chip : (m + 1) * chip, :] = top
            lo[m * chip : (m + 1) * chip, :] = (t - top.astype(F32)).astype(BF)
    for kx in range(NX):
        part = jnp.dot(hi[...], occ[kx], preferred_element_type=F32)
        part = (part + jnp.dot(lo[...], occ[kx], preferred_element_type=F32)) * scale
        for ky in range(NY):
            near[ky, kx] = part[ky * chip : (ky + 1) * chip]
            far[kx, ky] = part[(NY + ky) * chip : (NY + ky + 1) * chip]


def gamma_occ_kernel(c, s, hi, lo, b_all, *more):
    xi = s[0]
    base, out = more if len(more) > 1 else (None, *more)
    ni, na, nq = out.shape
    nqo = nq // (NX * NZL)
    picked = [slice((2 * i + c) * na, (2 * i + c + 1) * na) for i in range(ni)]
    hi_t, lo_t = hi[...].T, lo[...].T
    hi_t = jnp.concatenate([hi_t[p] for p in picked], axis=0)
    lo_t = jnp.concatenate([lo_t[p] for p in picked], axis=0)
    for xa in range(NX):
        b = b_all[(xi - xa) & (NX - 1)]
        rows = jnp.dot(hi_t, b, preferred_element_type=F32) + jnp.dot(lo_t, b, preferred_element_type=F32)
        for i in range(ni):
            block = rows[i * na : (i + 1) * na]
            for zl in range(NZL):
                q = (zl * NX + xa) * nqo
                part = block[:, zl * nqo : (zl + 1) * nqo]
                out[i, :, q : q + nqo] = part if base is None else part + base[i, :, q : q + nqo]


def tiles_kernel(nqo, s, near, far, out):
    zh = s[0]
    for h, half in enumerate((near, far)):
        for k in range(NZL):
            out[(zh ^ h) * NZL + k] = pack(half[:, k * nqo : (k + 1) * nqo])


def ring_gather(a, b, axis):
    a1, b3 = shift(a, axis, 1, 4), shift(b, axis, 3, 4)
    b1, a3 = shift(b, axis, 1, 4), shift(a, axis, 3, 4)
    a2, b2 = shift(a1, axis, 1, 4), shift(b3, axis, 3, 4)
    return [a, b, a1, b1, a2, b2, a3, b3]


def ring_sum(blocks, axis):
    def half(k, h):
        return blocks[k, 2 * h : 2 * h + 2]

    a2, b2 = shift(half(2, 0).astype(F16), axis, 3, 4), shift(half(2, 1).astype(F16), axis, 1, 4)
    b1, a3 = shift(half(1, 1).astype(F16), axis, 3, 4), shift(half(3, 0).astype(F16), axis, 1, 4)
    a1 = shift((half(1, 0) + a2.astype(F32)).astype(F16), axis, 3, 4)
    b3 = shift((half(3, 1) + b2.astype(F32)).astype(F16), axis, 1, 4)
    return (
        half(0, 0) + a1.astype(F32) + a3.astype(F32),
        half(0, 1) + b1.astype(F32) + b3.astype(F32),
    )


def sum_direct(blocks, axis):
    total = blocks[0].astype(F32)
    for k in (1, 3, 2):
        total = total + shift(blocks[k], axis, 4 - k, 4).astype(F32)
    return total


def whole(b_occ, b_outer, eps_occ, eps_outer, eps_vir):
    ni, na, nq = b_occ.shape
    nqo = b_outer.shape[2]
    core, xi, zh, y, _ = (lax.axis_index(n) for n in ("core", "x", "zh", "y", "zl"))
    wide = LANES * -(-(NZL * nqo + 2 * EXTRA) // LANES)
    chip = 2 * na
    rows, nv = ni * chip, NM * chip

    keep, give = call(
        message_kernel, [((na, nqo + EXTRA), BF)] * 2, [core], b_occ, b_outer, eps_vir.reshape(1, na)
    )
    got = lax.ppermute(give, "core", CORES)
    few = packed_rows(chip, nqo + EXTRA)
    (mine,) = call(pack_kernel, [((NZH * NZL, few, LANES), BF)], [core], keep, got)

    near, far = call(
        functools.partial(lay_out_kernel, nqo), [((chip, wide), BF)] * 2, [zh], exchange_z(mine)
    )

    near_x = [near] + [shift(near, "x", k, NX) for k in range(1, NX)]
    far_y = [far] + [shift(far, "y", k, NY) for k in range(1, NY)]
    near_all = ring_gather(jnp.stack(near_x[:2]), jnp.stack(near_x[2:]), "y")
    far_all = ring_gather(jnp.stack(far_y[:2]), jnp.stack(far_y[2:]), "x")

    other_rows = lax.ppermute(b_occ, "core", CORES)
    (occ_all,) = call(occ_kernel, [((NX, rows, wide), BF)], [xi], b_occ, other_rows)

    work = 2 * rows * nv * NX * wide
    eps_here = jnp.concatenate([eps_vir, jnp.sum(got[:, nqo : nqo + 3].astype(F32), axis=1)])
    eps_row = (eps_occ[:, None] - eps_here[None, :]).reshape(rows)

    b_all, amps_t, scaled, scales = call(
        lambda *refs: amps_kernel(ni, nqo, *refs),
        [((NX, nv, wide), BF), ((nv, rows), F32), ((NM, chip, rows), F32), ((8, LANES), F32)],
        [zh, y, core], *near_all, *far_all, occ_all, eps_row[None, :], eps_row[:, None], eps_outer[None, :],
        flops=work * 2,
    )
    swapped_t = lax.all_to_all(scaled.astype(F16), ("zh", "y"), 0, 0, tiled=True).astype(F32)
    hi, lo, near_p, far_p = call(
        tilde_kernel,
        [((nv, rows), BF)] * 2 + [((NY, NX, chip, wide), F32), ((NX, NY, chip, wide), F32)],
        [zh, y, core], amps_t, swapped_t, occ_all, scales,
        flops=work * 2,
    )

    near_a, near_b = ring_sum(near_p, "y")
    far_a, far_b = ring_sum(far_p, "x")
    near_s = [(p[k] * 0.25).astype(F16) for p in (near_a, near_b) for k in range(2)]
    far_s = [(p[k] * 0.25).astype(F16) for p in (far_a, far_b) for k in range(2)]
    near_t, far_t = sum_direct(near_s, "x") * 0.25, sum_direct(far_s, "y") * 0.25

    (given,) = call(
        functools.partial(gamma_occ_kernel, 1), [((ni, na, nq), F32)], [xi], hi, lo, b_all, flops=work
    )
    given = lax.ppermute(given, "core", CORES)
    (gamma_occ,) = call(
        functools.partial(gamma_occ_kernel, 0), [((ni, na, nq), F32)], [xi], hi, lo, b_all, given, flops=work
    )

    small = (NZH * NZL, packed_rows(chip, nqo), LANES)
    (tiles,) = call(functools.partial(tiles_kernel, nqo), [(small, F32)], [zh], near_t, far_t)
    arrived = exchange_z(tiles.astype(F16))
    mine_j, give_j = call(
        section_kernel, [((na, nqo), F32)] * 2, [core], arrived.astype(F32).sum(0), scales
    )
    other_j = lax.ppermute(give_j, "core", CORES)
    gamma_outer = jnp.where(core == 0, jnp.stack([mine_j, other_j]), jnp.stack([other_j, mine_j]))
    return (gamma_occ, gamma_outer)


def solution(mesh):
    fine = Mesh(mesh.devices.reshape(SIZES), AXES)
    occ, vir = ("zl", "x"), ("zh", "y", "core")
    return jax.shard_map(
        whole,
        mesh=fine,
        in_specs=(P(occ, vir, None), P(None, vir, occ), P(occ), P(), P(vir)),
        out_specs=(P(occ, vir, None), P(None, vir, occ)),
        check_vma=False,
    )
```

```python
import functools
import math

import jax
import jax.numpy as jnp
from jax import lax
from jax.experimental import pallas as pl
from jax.experimental.pallas import tpu as pltpu
from jax.sharding import Mesh
from jax.sharding import PartitionSpec as P


AXES = ("zl", "x", "zh", "y", "core")
SIZES = (4, 4, 2, 4, 2)
NX, NY, NZL, NZH = 4, 4, 4, 2
NM = NZH * NY
BF, F16, F32 = jnp.bfloat16, jnp.float16, jnp.float32
EXTRA = 16
OCC_TOP, OUTER_TOP = 3, 4
LANES = 128
LIMIT = 28
SMEM = pl.BlockSpec(memory_space=pltpu.SMEM)
VMEM = pl.BlockSpec(memory_space=pltpu.VMEM)
CORES = [(0, 1), (1, 0)]


def call(kernel, outs, scalars, *arrays, flops=0, scratch=()):
    moved = sum(a.size * a.dtype.itemsize for a in arrays) + sum(4 * math.prod(s) for s, _ in outs)
    return pl.pallas_call(
        kernel,
        out_shape=[jax.ShapeDtypeStruct(s, d) for s, d in outs],
        in_specs=[SMEM] + [VMEM] * len(arrays),
        out_specs=[VMEM] * len(outs),
        scratch_shapes=list(scratch),
        cost_estimate=pl.CostEstimate(flops=flops, bytes_accessed=moved, transcendentals=0),
        compiler_params=pltpu.CompilerParams(vmem_limit_bytes=LIMIT * 2**20),
    )(jnp.stack(scalars).astype(jnp.int32), *arrays)


def shift(array, axis, k, size):
    return lax.ppermute(array, axis, [(p, (p + k) % size) for p in range(size)])


def exchange_z(array):
    return lax.all_to_all(array, ("zh", "zl"), 0, 0, tiled=True)


def nt(a, b):
    return lax.dot_general(a, b, (((1,), (1,)), ((), ())), preferred_element_type=F32)


def message_kernel(s, occ, outer, eps, keep, give):
    core = s[0]
    occ_top = jnp.max(jnp.abs(occ[...].astype(F32)))
    n = eps.shape[1]
    here = lax.broadcasted_iota(jnp.int32, (n, n), 0) == lax.broadcasted_iota(jnp.int32, (n, n), 1)
    e = jnp.sum(jnp.where(here, eps[...], 0.0), axis=1, keepdims=True)
    parts = []
    for _ in range(3):
        part = e.astype(BF).astype(F32)
        parts.append(part)
        e = e - part
    na, nqo = outer.shape[1:]
    lane = lax.broadcasted_iota(jnp.int32, (na, EXTRA), 1)
    for out, j in ((keep, core), (give, 1 - core)):
        rows = outer[j]
        row_top = jnp.max(jnp.abs(rows.astype(F32)), axis=1, keepdims=True)
        side = jnp.where(lane == OCC_TOP, occ_top, 0.0)
        for n, part in enumerate(parts):
            side = jnp.where(lane == n, part, side)
        side = jnp.where(lane == OUTER_TOP, row_top, side)
        out[:, :nqo] = rows
        out[:, nqo:] = side.astype(BF)


def groups(rows, width):
    fit = [g for g in range(LANES // width, 0, -1) if rows % g == 0]
    return next((g for g in fit if rows // g % 8 == 0), fit[0])


def packed_rows(rows, width):
    return rows + rows // groups(rows, width - LANES)


def pack(block):
    rows, few = block.shape[0], block.shape[1] - LANES
    n = groups(rows, few)
    each = rows // n
    tail = [block[g * each : (g + 1) * each, LANES:] for g in range(n)]
    if n * few < LANES:
        tail.append(jnp.zeros((each, LANES - n * few), F32))
    return jnp.concatenate([block[:, :LANES], jnp.concatenate(tail, axis=1)], axis=0)


def unpack(packed, rows, width):
    few = width - LANES
    n = groups(rows, few)
    tail = jnp.concatenate([packed[rows:, g * few : (g + 1) * few] for g in range(n)], axis=0)
    return jnp.concatenate([packed[:rows], tail], axis=1)


def pack_kernel(s, keep, got, out):
    block = pack(jnp.concatenate([keep[...].astype(F32), got[...].astype(F32)], axis=0)).astype(BF)
    out[...] = block


def section_kernel(s, packed, scales, keep, give):
    na, width = keep.shape
    block = unpack(packed[...] * (16.0 * scales[3:4, 0:1]), 2 * na, width)
    keep[...] = block[:na]
    give[...] = block[na:]


def lay_out_kernel(nqo, s, z, near, far):
    zh = s[0]
    rows, wide = near.shape
    for out, half in ((near, zh), (far, 1 - zh)):
        blocks = [unpack(z[half * NZL + k].astype(F32), rows, nqo + EXTRA) for k in range(NZL)]
        most = blocks[0][:, nqo:]
        for b in blocks[1:]:
            most = jnp.maximum(most, b[:, nqo:])
        used = NZL * nqo + 2 * EXTRA
        out[...] = jnp.concatenate(
            [b[:, :nqo] for b in blocks] + [blocks[0][:, nqo:], most, jnp.zeros((rows, wide - used), F32)], axis=1
        ).astype(BF)


def occ_kernel(s, own, other, out):
    xi = s[0]
    ni, na, nq = own.shape
    nqo, wide = nq // (NX * NZL), out.shape[2]
    for xa in range(NX):
        kx = (xi - xa) & (NX - 1)
        for i in range(ni):
            for c, src in enumerate((own, other)):
                cols = [src[i, :, (zl * NX + xa) * nqo : (zl * NX + xa + 1) * nqo] for zl in range(NZL)]
                cols.append(jnp.zeros((na, wide - NZL * nqo), BF))
                at = (2 * i + c) * na
                out[kx, at : at + na, :] = jnp.concatenate(cols, axis=1)


def amps_kernel(ni, nqo, s, *refs):
    zh, y = s[0], s[1]
    near, far, (occ, eps_lane, eps_sub, eps_outer, b_all, at, send, scales) = refs[:8], refs[8:16], refs[16:]
    chip = near[0].shape[1]
    half = NY * chip
    for k in range(4):
        for other in range(4):
            b_all[other, k * chip : (k + 1) * chip, :] = near[2 * k + other // 2][other % 2]
            at_row = half + other * chip
            b_all[k, at_row : at_row + chip, :] = far[2 * k + other // 2][other % 2]
    tile = NZL * nqo // LANES * LANES
    off = NZL * nqo - tile
    tail = b_all[0, :, tile : tile + LANES].astype(F32)
    eps_b_sub = tail[:, off : off + 1] + tail[:, off + 1 : off + 2] + tail[:, off + 2 : off + 3]
    lane8 = lax.broadcasted_iota(jnp.int32, (8, LANES), 1)
    pick = jnp.where((lane8 >= off) & (lane8 < off + 3), 1.0, 0.0).astype(BF)
    eps_b_lane = nt(pick, b_all[0, :, tile : tile + LANES])[0:1]
    most = jnp.max(tail, axis=0, keepdims=True)
    for kx in range(1, NX):
        most = jnp.maximum(most, jnp.max(b_all[kx, :, tile : tile + LANES].astype(F32), axis=0, keepdims=True))
    lane1 = lax.broadcasted_iota(jnp.int32, (1, LANES), 1)

    def extra(n):
        return jnp.sum(jnp.where(lane1 == off + EXTRA + n, most, 0.0), axis=1, keepdims=True)

    nq = NX * NZL * nqo
    amp_top = jnp.maximum(nq * extra(OCC_TOP) * extra(OUTER_TOP), 1e-30)
    sum_top = jnp.maximum(3.0 * ni * chip * amp_top * extra(OCC_TOP), 1e-30)
    amp_scale, sum_scale = 60000.0 / amp_top, 15000.0 / sum_top
    for n, value in enumerate((amp_scale, amp_top / 60000.0, sum_scale, sum_top / 15000.0)):
        scales[n : n + 1, :] = jnp.broadcast_to(value, (1, LANES))

    total = nt(occ[0], b_all[0])
    total_t = nt(b_all[0], occ[0])
    for kx in range(1, NX):
        total = total + nt(occ[kx], b_all[kx])
        total_t = total_t + nt(b_all[kx], occ[kx])
    eps_j = jnp.where(s[2] == 0, eps_outer[0:1, 0:1], eps_outer[0:1, 1:2])
    at[...] = total_t / (eps_lane[...] + eps_j - eps_b_sub)
    scaled = total / (eps_sub[...] + eps_j - eps_b_lane) * amp_scale
    for h in range(NZH):
        for k in range(NY):
            m, to = h * NY + k, (zh ^ h) * NY + ((y - k) & (NY - 1))
            send[to] = jnp.concatenate(
                [scaled[i * chip : (i + 1) * chip, m * chip : (m + 1) * chip] for i in range(ni)], axis=1
            )


def tilde_kernel(s, at, st, occ, scales, hi, lo, near, far):
    zh, y = s[0], s[1]
    chip = st.shape[1]
    back, scale = scales[1:2, 0:1], scales[2:3, 0:1]
    for h in range(NZH):
        for k in range(NY):
            m, to = h * NY + k, (zh ^ h) * NY + ((y - k) & (NY - 1))
            t = 2.0 * at[m * chip : (m + 1) * chip, :] - st[to] * back
            top = t.astype(BF)
            hi[m * chip : (m + 1) * chip, :] = top
            lo[m * chip : (m + 1) * chip, :] = (t - top.astype(F32)).astype(BF)
    for kx in range(NX):
        part = jnp.dot(hi[...], occ[kx], preferred_element_type=F32)
        part = (part + jnp.dot(lo[...], occ[kx], preferred_element_type=F32)) * scale
        for ky in range(NY):
            near[ky, kx] = part[ky * chip : (ky + 1) * chip]
            far[kx, ky] = part[(NY + ky) * chip : (NY + ky + 1) * chip]


def gamma_occ_kernel(c, s, hi, lo, b_all, *more):
    xi = s[0]
    base, out = more if len(more) > 1 else (None, *more)
    ni, na, nq = out.shape
    nqo = nq // (NX * NZL)
    picked = [slice((2 * i + c) * na, (2 * i + c + 1) * na) for i in range(ni)]
    hi_t, lo_t = hi[...].T, lo[...].T
    hi_t = jnp.concatenate([hi_t[p] for p in picked], axis=0)
    lo_t = jnp.concatenate([lo_t[p] for p in picked], axis=0)
    for xa in range(NX):
        b = b_all[(xi - xa) & (NX - 1)]
        rows = jnp.dot(hi_t, b, preferred_element_type=F32) + jnp.dot(lo_t, b, preferred_element_type=F32)
        for i in range(ni):
            block = rows[i * na : (i + 1) * na]
            for zl in range(NZL):
                q = (zl * NX + xa) * nqo
                part = block[:, zl * nqo : (zl + 1) * nqo]
                out[i, :, q : q + nqo] = part if base is None else part + base[i, :, q : q + nqo]


def tiles_kernel(nqo, s, near, far, out):
    zh = s[0]
    for h, half in enumerate((near, far)):
        for k in range(NZL):
            out[(zh ^ h) * NZL + k] = pack(half[:, k * nqo : (k + 1) * nqo])


def ring_gather(a, b, axis):
    a1, b3 = shift(a, axis, 1, 4), shift(b, axis, 3, 4)
    b1, a3 = shift(b, axis, 1, 4), shift(a, axis, 3, 4)
    a2, b2 = shift(a1, axis, 1, 4), shift(b3, axis, 3, 4)
    return [a, b, a1, b1, a2, b2, a3, b3]


def ring_sum(blocks, axis):
    def half(k, h):
        return blocks[k, 2 * h : 2 * h + 2]

    a2, b2 = shift(half(2, 0).astype(F16), axis, 3, 4), shift(half(2, 1).astype(F16), axis, 1, 4)
    b1, a3 = shift(half(1, 1).astype(F16), axis, 3, 4), shift(half(3, 0).astype(F16), axis, 1, 4)
    a1 = shift((half(1, 0) + a2.astype(F32)).astype(F16), axis, 3, 4)
    b3 = shift((half(3, 1) + b2.astype(F32)).astype(F16), axis, 1, 4)
    return (
        half(0, 0) + a1.astype(F32) + a3.astype(F32),
        half(0, 1) + b1.astype(F32) + b3.astype(F32),
    )


def sum_direct(blocks, axis):
    total = blocks[0].astype(F32)
    for k in (1, 3, 2):
        total = total + shift(blocks[k], axis, 4 - k, 4).astype(F32)
    return total


def whole(b_occ, b_outer, eps_occ, eps_outer, eps_vir):
    ni, na, nq = b_occ.shape
    nqo = b_outer.shape[2]
    core, xi, zh, y, _ = (lax.axis_index(n) for n in ("core", "x", "zh", "y", "zl"))
    wide = LANES * -(-(NZL * nqo + 2 * EXTRA) // LANES)
    chip = 2 * na
    rows, nv = ni * chip, NM * chip

    keep, give = call(
        message_kernel, [((na, nqo + EXTRA), BF)] * 2, [core], b_occ, b_outer, eps_vir.reshape(1, na)
    )
    got = lax.ppermute(give, "core", CORES)
    few = packed_rows(chip, nqo + EXTRA)
    (mine,) = call(pack_kernel, [((few, LANES), BF)], [core], keep, got)

    near, far = call(
        functools.partial(lay_out_kernel, nqo), [((chip, wide), BF)] * 2, [zh], lax.all_gather(mine, ("zh", "zl"))
    )

    near_x = [near] + [shift(near, "x", k, NX) for k in range(1, NX)]
    far_y = [far] + [shift(far, "y", k, NY) for k in range(1, NY)]
    near_all = ring_gather(jnp.stack(near_x[:2]), jnp.stack(near_x[2:]), "y")
    far_all = ring_gather(jnp.stack(far_y[:2]), jnp.stack(far_y[2:]), "x")

    other_rows = lax.ppermute(b_occ, "core", CORES)
    (occ_all,) = call(occ_kernel, [((NX, rows, wide), BF)], [xi], b_occ, other_rows)

    work = 2 * rows * nv * NX * wide
    eps_here = jnp.concatenate([eps_vir, jnp.sum(got[:, nqo : nqo + 3].astype(F32), axis=1)])
    eps_row = (eps_occ[:, None] - eps_here[None, :]).reshape(rows)

    b_all, amps_t, scaled, scales = call(
        lambda *refs: amps_kernel(ni, nqo, *refs),
        [((NX, nv, wide), BF), ((nv, rows), F32), ((NM, chip, rows), F32), ((8, LANES), F32)],
        [zh, y, core], *near_all, *far_all, occ_all, eps_row[None, :], eps_row[:, None], eps_outer[None, :],
        flops=work * 2,
    )
    swapped_t = lax.all_to_all(scaled.astype(F16), ("zh", "y"), 0, 0, tiled=True).astype(F32)
    hi, lo, near_p, far_p = call(
        tilde_kernel,
        [((nv, rows), BF)] * 2 + [((NY, NX, chip, wide), F32), ((NX, NY, chip, wide), F32)],
        [zh, y, core], amps_t, swapped_t, occ_all, scales,
        flops=work * 2,
    )

    near_a, near_b = ring_sum(near_p, "y")
    far_a, far_b = ring_sum(far_p, "x")
    near_s = [(p[k] * 0.25).astype(F16) for p in (near_a, near_b) for k in range(2)]
    far_s = [(p[k] * 0.25).astype(F16) for p in (far_a, far_b) for k in range(2)]
    near_t, far_t = sum_direct(near_s, "x") * 0.25, sum_direct(far_s, "y") * 0.25

    (given,) = call(
        functools.partial(gamma_occ_kernel, 1), [((ni, na, nq), F32)], [xi], hi, lo, b_all, flops=work
    )
    given = lax.ppermute(given, "core", CORES)
    (gamma_occ,) = call(
        functools.partial(gamma_occ_kernel, 0), [((ni, na, nq), F32)], [xi], hi, lo, b_all, given, flops=work
    )

    small = (NZH * NZL, packed_rows(chip, nqo), LANES)
    (tiles,) = call(functools.partial(tiles_kernel, nqo), [(small, F32)], [zh], near_t, far_t)
    arrived = exchange_z(tiles.astype(F16))
    mine_j, give_j = call(
        section_kernel, [((na, nqo), F32)] * 2, [core], arrived.astype(F32).sum(0), scales
    )
    other_j = lax.ppermute(give_j, "core", CORES)
    gamma_outer = jnp.where(core == 0, jnp.stack([mine_j, other_j]), jnp.stack([other_j, mine_j]))
    return (gamma_occ, gamma_outer)


def solution(mesh):
    fine = Mesh(mesh.devices.reshape(SIZES), AXES)
    occ, vir = ("zl", "x"), ("zh", "y", "core")
    return jax.shard_map(
        whole,
        mesh=fine,
        in_specs=(P(occ, vir, None), P(None, vir, occ), P(occ), P(), P(vir)),
        out_specs=(P(occ, vir, None), P(None, vir, occ)),
        check_vma=False,
    )
```
